32 devices in a mesh: seq: 8 (over y, x, core), head: 4 (over z).
Axes of the slice: x: 2, y: 2, z: 4, core: 2. Of those that a mesh axis runs over, the one named last changes fastest.
Arguments:
- values: bfloat16 [16384, 5120], P('seq', 'head'), may hold values from -6 to 6
- gates: bfloat16 [16384, 5120], P('seq', 'head'), may hold values from -6 to 6
- b_proj: bfloat16 [16384, 128], P('seq'), may hold values from -2 to 2
- c_proj: bfloat16 [16384, 128], P('seq'), may hold values from -2 to 2
- step_size: float32 [80, 16384], P('head', 'seq'), may hold values from 0.006 to 0.06
- decay_rate: float32 [80, 16384], P('head', 'seq'), may hold values from 0 to 1.2, as said below
- skip_gain: float32 [80], P('head'), may hold values from 0.5 to 2
- norm_gain: float32 [5120], P('head'), may hold values from 0.25 to 1.75
- readout_matrix: bfloat16 [5120, 2560], P('head'), may hold values from -0.078125 to 0.078125
- span_counts: int32 [8], P('seq'), may hold values from 1 to 8, as said below
- remaining_count: int32 [8], P('seq'), may hold values from 1 to 256
Outputs:
- mixer_response: bfloat16 [16384, 2560], P(('seq', 'head'))
The draws below stay inside these ranges and needn't reach their ends.
Inputs may be any that keep to these rules, and one draw needn't show every extreme that they name: `span_counts`: some shard uses all 8 span slots in every draw. `decay_rate`: Positive.
All inputs are finite; a program needn't handle non-finite values.
Results may differ from the reference program's by a relative error of at most 0.02.
Values may be sent and summed in bfloat16 or wider, within the bound.
A program may use at most 192 MiB of HBM per device.

```python
import math
import jax
import jax.numpy as jnp
from jax import lax

D = 2560
HEADS = 80
P_SIZE = 64
N = 128
SPAN = 256
CH_DEV = 8
TOK_DEV = 2048
SHARDS = 8
ENTRY_CAPACITY = 16384
N_HEAD = 4


def draw_decay_rate(key, part):
    keys = jax.random.split(key, 6)
    share = 0.5
    quick_heads = jax.random.uniform(keys[0], (HEADS,)) < share
    quick = jnp.exp(jax.random.uniform(keys[1], (HEADS,), jnp.float32, math.log(1.0 / 50.0), math.log(1.0 / 30.0)))
    slow = 0.2 * math.log(10.0) / ENTRY_CAPACITY * jnp.exp(jax.random.uniform(keys[2], (HEADS,), jnp.float32, -0.5, 0.5))
    base = jnp.where(quick_heads, quick, slow)
    blockwise = jnp.exp(jax.random.uniform(keys[3], (HEADS, ENTRY_CAPACITY // SPAN, 1), jnp.float32, -0.7, 0.7))
    rough = jax.random.uniform(keys[4], (HEADS, ENTRY_CAPACITY // SPAN, SPAN), jnp.float32, 0.5, 2.0)
    forgetting_factor = (base[:, None, None] * blockwise * rough).reshape(HEADS, ENTRY_CAPACITY)
    entry_indices = jax.random.randint(keys[5], (3,), 0, ENTRY_CAPACITY)
    element_cluster = jnp.zeros((ENTRY_CAPACITY,), jnp.float32).at[entry_indices].add(0.3)
    return (forgetting_factor + element_cluster[None, :]).astype(jnp.float32)


def draw_span_counts(key, part):
    first_key, second_key = jax.random.split(key)
    first = jax.random.randint(first_key, (SHARDS,), 0, CH_DEV)
    second = jax.random.randint(second_key, (SHARDS,), 0, CH_DEV)
    counts = 1 + first * second // (CH_DEV - 1)
    chosen = jax.random.randint(jax.random.fold_in(key, 7), (), 0, SHARDS)
    return counts.at[chosen].set(CH_DEV).astype(jnp.int32)


def place_ends(values, key, least, high):
    shape = values.shape
    place = [jax.random.randint(jax.random.fold_in(key, axis), (), 0, shape[axis]) for axis in range(len(shape))]
    values = values.at[tuple(place)].set(least)
    longest = shape.index(max(shape))
    place[longest] = (place[longest] + 1) % shape[longest]
    return values.at[tuple(place)].set(high)


def level_of(own_key, extent, pieces, low, high):
    loudness, own = 1.0, jax.random.fold_in(own_key, 6)
    for position, shards_of in pieces:
        heights = jnp.exp(jax.random.uniform(jax.random.fold_in(own, position), (shards_of,), jnp.float32, low / len(pieces), high / len(pieces)))
        loudness = loudness * jnp.repeat(heights, extent[position] // shards_of).reshape([-1 if axis == position else 1 for axis in range(len(extent))])
    return loudness


def gaussian(key, dims, scale, reach, pieces=(), kind=jnp.bfloat16):
    values = jax.random.normal(key, dims, jnp.float32) * scale
    if len(pieces) > 0:
        values = level_of(key, dims, pieces, -0.22, 0.18) * values
    return jnp.clip(values, min=-reach, max=reach).astype(kind)


def setup_inputs(seed: int = 0) -> dict:
    seeds = jax.random.split(jax.random.key(seed), 12)
    values = gaussian(seeds[0], (ENTRY_CAPACITY, HEADS * P_SIZE), 1.0, 6.0, ((0, 8), (1, 4)))
    gates = gaussian(seeds[1], (ENTRY_CAPACITY, HEADS * P_SIZE), 1.0, 6.0, ((0, 8), (1, 4)))
    b_proj = gaussian(seeds[2], (ENTRY_CAPACITY, N), 0.3, 2.0, ((0, 8),))
    c_proj = gaussian(seeds[3], (ENTRY_CAPACITY, N), 0.3, 2.0, ((0, 8),))
    step_size = jnp.clip(jnp.exp(math.log(0.06) - 2.3025851 * jax.random.uniform(seeds[4], (HEADS, ENTRY_CAPACITY), jnp.float32) ** level_of(seeds[4], (HEADS, ENTRY_CAPACITY), ((0, 4), (1, 8)), -0.2, 0.2)), 0.006, 0.06)
    decay_rate = draw_decay_rate(jax.random.fold_in(seeds[11], 71), 0)
    skip_gain = jnp.clip(0.5 + 1.5 * jax.random.uniform(seeds[6], (HEADS,), jnp.float32) ** level_of(seeds[6], (HEADS,), ((0, 4),), -0.2, 0.2), 0.5, 2.0)
    norm_gain = jnp.clip(1.0 + 0.15 * jax.random.normal(seeds[7], (HEADS * P_SIZE,), jnp.float32), 0.25, 1.75)
    readout_matrix = gaussian(seeds[8], (HEADS * P_SIZE, D), (HEADS * P_SIZE) ** -0.5, 0.078125, ((0, 4),))
    span_counts = draw_span_counts(jax.random.fold_in(seeds[11], 71), 0)
    remaining_count = place_ends(jax.random.randint(seeds[10], (SHARDS,), 1, SPAN + 1), jax.random.fold_in(seeds[10], 1), 1, SPAN).astype(jnp.int32)
    return {"values": values, "gates": gates, "b_proj": b_proj, "c_proj": c_proj, "step_size": step_size, "decay_rate": decay_rate, "skip_gain": skip_gain, "norm_gain": norm_gain, "readout_matrix": readout_matrix, "span_counts": span_counts, "remaining_count": remaining_count}


def reference(values, gates, b_proj, c_proj, step_size, decay_rate, skip_gain, norm_gain, readout_matrix, span_counts, remaining_count):
    f32 = jnp.float32
    bf16 = jnp.bfloat16
    valid = (span_counts - 1) * SPAN + remaining_count
    limit = jnp.repeat(valid, TOK_DEV)
    positioned_entries = jnp.arange(ENTRY_CAPACITY, dtype=jnp.int32) % TOK_DEV
    live = (positioned_entries < limit).astype(f32)
    blocks = ENTRY_CAPACITY // SPAN

    def spanned(array):
        return array.reshape((blocks, SPAN) + array.shape[1:])

    def per_head(array):
        return array.reshape(HEADS, blocks, SPAN).transpose(1, 0, 2)
    items = (spanned(values), spanned(gates), spanned(b_proj), spanned(c_proj), per_head(step_size), per_head(decay_rate), spanned(live))
    lower = jnp.arange(SPAN)[:, None] >= jnp.arange(SPAN)[None, :]
    group_width = HEADS * P_SIZE // N_HEAD

    def advance(state, item):
        x_span, z_span, b_span, c_span, dt_span, rate_span, live_span = item
        logdec = -rate_span * live_span[None, :]
        running = jnp.cumsum(logdec, axis=1)
        weight = dt_span * live_span[None, :]
        gram = jnp.einsum('in,jn->ij', c_span.astype(f32), b_span.astype(f32))
        spread = jnp.where(lower[None], running[:, :, None] - running[:, None, :], -1e+30)
        mixing = lax.optimization_barrier((gram[None] * jnp.exp(spread) * weight[:, None, :]).astype(bf16))
        heads_x = x_span.reshape(SPAN, HEADS, P_SIZE).astype(f32)
        inner = jnp.einsum('hij,jhp->ihp', mixing.astype(f32), heads_x)
        held = lax.optimization_barrier(state.astype(bf16))
        carried = jnp.einsum('in,hpn->ihp', c_span.astype(f32), held.astype(f32)) * jnp.exp(running).T[:, :, None]
        mixed = (inner + carried + skip_gain[None, :, None] * heads_x) * live_span[:, None, None]
        tail = jnp.exp(running[:, -1:] - running) * weight
        weighted = lax.optimization_barrier((heads_x * tail.T[:, :, None]).astype(bf16))
        fresh = jnp.einsum('jhp,jn->hpn', weighted.astype(f32), b_span.astype(f32))
        state = jnp.exp(running[:, -1])[:, None, None] * state + fresh
        gated = mixed.reshape(SPAN, HEADS * P_SIZE) * jax.nn.silu(z_span.astype(f32))
        meansq = lax.optimization_barrier(jnp.mean(gated * gated, axis=1, keepdims=True))
        normed = (gated * lax.rsqrt(meansq + 1e-05) * norm_gain[None, :]).astype(bf16)
        summed = jnp.zeros((SPAN, D), f32)
        for group in range(N_HEAD):
            lo_col = group * group_width
            partial_term = jnp.dot(normed[:, lo_col:lo_col + group_width], readout_matrix[lo_col:lo_col + group_width], preferred_element_type=f32).astype(bf16)
            summed = summed + lax.optimization_barrier(partial_term).astype(f32)
        return (state, summed.astype(bf16))
    start_state = jnp.zeros((HEADS, P_SIZE, N), f32)
    _, produced = lax.scan(advance, start_state, items)
    return produced.reshape(ENTRY_CAPACITY, D)
```

```python
import functools
import math

import jax
import jax.numpy as jnp
from jax import lax
from jax.experimental import pallas as pl
from jax.experimental.pallas import tpu as pltpu
from jax.sharding import PartitionSpec as P

SPAN = 256
LOG2E = math.log2(math.e)
F32 = jnp.float32
BF16 = jnp.bfloat16
HIGH = lax.Precision.HIGHEST
MESH = pl.DeviceIdType.MESH
VMEM = pltpu.VMEM
LIMIT = 63 * 1024 * 1024
TILE = 256


def contract(a, b, da, db, precision=None):
    return lax.dot_general(
        a, b, (((da,), (db,)), ((), ())), precision=precision, preferred_element_type=F32
    )


def expander(heads, width):
    size = width // heads
    col = lax.broadcasted_iota(jnp.int32, (heads, width), 1) // size
    row = lax.broadcasted_iota(jnp.int32, (heads, width), 0)
    return jnp.where(col == row, 1.0, 0.0).astype(F32)


def halves(a):
    hi = a.astype(BF16)
    return hi, (a - hi.astype(F32)).astype(BF16)


def pack_rows(total):
    total = jnp.broadcast_to(total, (16, total.shape[1]))
    hi, mid = halves(total)
    low = (total - hi.astype(F32) - mid.astype(F32)).astype(BF16)
    row = lax.broadcasted_iota(jnp.int32, total.shape, 0)
    parts = jnp.where(row == 0, hi.astype(F32), jnp.where(row == 1, mid.astype(F32), low.astype(F32)))
    return jnp.where(row < 3, parts, 0.0).astype(BF16)


def unpack_rows(rows):
    rows = rows.astype(F32)
    return rows[0:1, :] + rows[1:2, :] + rows[2:3, :]


def pick(table, index):
    total = jnp.int32(0)
    for i, value in enumerate(table):
        total = total + jnp.where(index == i, jnp.int32(value), jnp.int32(0))
    return total


def near_order(ranks):
    return [sorted((r for r in range(ranks) if r != h), key=lambda r: (abs(r - h), r)) for h in range(ranks)]


def layer_kernel(
    ranks,
    shards,
    count_ref,
    remain_ref,
    skip_ref,
    gain_ref,
    x_hbm,
    g_hbm,
    b_hbm,
    c_hbm,
    st_hbm,
    dr_hbm,
    w_hbm,
    out_hbm,
    x_ref,
    g_ref,
    b_ref,
    c_ref,
    st_ref,
    dr_ref,
    runT_ref,
    q_ref,
    before_ref,
    lead_ref,
    s_ref,
    l_ref,
    mine_ref,
    other_ref,
    chip_ref,
    chips_ref,
    inc_ref,
    w_ref,
    got_ref,
    ss_buf,
    ss_ref,
    acc_ref,
    res_ref,
    x_sem,
    g_sem,
    in_sem,
    w_sem,
    right_s,
    right_r,
    left_s,
    left_r,
    plane_s,
    plane_r,
    sib_s,
    sib_r,
    pair_s,
    pair_r,
    chip_s,
    chip_r,
    send_sem,
    recv_sem,
    ssend_sem,
    srecv_sem,
    out_sem,
):
    heads, length = q_ref.shape
    width = x_ref.shape[1]
    blocks = length // SPAN
    each = blocks // ranks
    share = length // ranks
    state = s_ref.shape[0]
    depth = res_ref.shape[1]
    rows = width // shards
    chips = shards // 2
    half = width // 2
    tiles = depth // TILE
    me = lax.axis_index("head")
    place = lax.axis_index("seq")
    core = lax.rem(place, 2)
    chip = lax.div(place, 2)
    sibling = place + 1 - 2 * core
    valid = (count_ref[0] - 1) * SPAN + remain_ref[0]

    def span_at(c):
        return pl.ds(pl.multiple_of(c * SPAN, SPAN), SPAN)

    def slice_at(owner):
        return pl.ds(pl.multiple_of(owner * rows, rows), rows)

    def load_w(i):
        owner = lax.rem(place + i, shards)
        return pltpu.make_async_copy(
            w_hbm.at[slice_at(owner), :], w_ref.at[me, slice_at(owner), :], w_sem.at[i]
        )

    def load_x(c):
        return pltpu.make_async_copy(x_hbm.at[span_at(c), :], x_ref.at[span_at(c), :], x_sem.at[c])

    def load_g(c):
        return pltpu.make_async_copy(g_hbm.at[span_at(c), :], g_ref.at[span_at(c), :], g_sem.at[c])

    smalls = [
        pltpu.make_async_copy(src, dst, in_sem.at[i])
        for i, (src, dst) in enumerate(
            ((st_hbm, st_ref), (dr_hbm, dr_ref), (b_hbm, b_ref), (c_hbm, c_ref))
        )
    ]

    def along(k, step):
        r = me - step * k
        send, recv = (right_s, right_r) if step > 0 else (left_s, left_r)
        return pltpu.make_async_remote_copy(
            src_ref=w_ref.at[r, slice_at(place), :],
            dst_ref=w_ref.at[r, slice_at(place), :],
            send_sem=send.at[k],
            recv_sem=recv.at[k],
            device_id={"head": me + step},
            device_id_type=MESH,
        )

    def arrived(k, step):
        r = me - step * (k + 1)
        send, recv = (right_s, right_r) if step > 0 else (left_s, left_r)
        return pltpu.make_async_remote_copy(
            src_ref=w_ref.at[r, slice_at(place), :],
            dst_ref=w_ref.at[r, slice_at(place), :],
            send_sem=send.at[k],
            recv_sem=recv.at[k],
            device_id={"head": me - step},
            device_id_type=MESH,
        )

    def plane(r, j):
        slot = lax.rem(r - me + ranks, ranks) - 1
        dest = lax.rem(chip + j, chips) * 2 + core
        return pltpu.make_async_remote_copy(
            src_ref=w_ref.at[r, slice_at(place), :],
            dst_ref=w_ref.at[r, slice_at(place), :],
            send_sem=plane_s.at[slot, j],
            recv_sem=plane_r.at[slot, j],
            device_id={"seq": dest},
            device_id_type=MESH,
        )

    def landed(r, j):
        slot = lax.rem(r - me + ranks, ranks) - 1
        owner = lax.rem(chip - j + chips, chips) * 2 + core
        return pltpu.make_async_remote_copy(
            src_ref=w_ref.at[r, slice_at(owner), :],
            dst_ref=w_ref.at[r, slice_at(owner), :],
            send_sem=plane_s.at[slot, j],
            recv_sem=plane_r.at[slot, j],
            device_id={"seq": owner},
            device_id_type=MESH,
        )

    def across(r, j, of_core):
        slot = lax.rem(r - me + ranks, ranks) - 1
        owner = lax.rem(chip - j + chips, chips) * 2 + of_core
        return pltpu.make_async_remote_copy(
            src_ref=w_ref.at[r, slice_at(owner), :],
            dst_ref=w_ref.at[r, slice_at(owner), :],
            send_sem=sib_s.at[slot, j],
            recv_sem=sib_r.at[slot, j],
            device_id={"seq": sibling},
            device_id_type=MESH,
        )

    def spread_plane(r):
        across(r, 0, core).start()

        def one(j, carry):
            plane(r, j).start()
            return carry

        lax.fori_loop(1, chips, one, 0)

    def relay(k):
        for step in (1, -1):
            source = me - step * k
            last = me == (ranks - 1 if step > 0 else 0)

            @pl.when((source >= 0) & (source < ranks))
            def _(step=step, source=source, last=last):
                arrived(k - 1, step).wait_recv()
                if k < ranks - 1:

                    @pl.when(jnp.logical_not(last))
                    def _():
                        along(k, step).start()

                spread_plane(source)

    load_w(0).start()
    for copy in smalls[:3]:
        copy.start()

    def load_xs(c, carry):
        load_x(c).start()
        return carry

    lax.fori_loop(0, blocks, load_xs, 0)
    smalls[3].start()

    barrier = pltpu.get_barrier_semaphore()

    def greet(k, carry):
        pl.semaphore_signal(
            barrier, inc=1, device_id={"head": lax.rem(me + k, ranks)}, device_id_type=MESH
        )
        return carry

    def greet_plane(j, carry):
        dest = lax.rem(chip + j, chips) * 2 + core
        pl.semaphore_signal(barrier, inc=1, device_id={"seq": dest}, device_id_type=MESH)
        return carry

    lax.fori_loop(1, ranks, greet, 0)
    lax.fori_loop(1, chips, greet_plane, 0)
    pl.semaphore_signal(barrier, inc=1, device_id={"seq": sibling}, device_id_type=MESH)
    pl.semaphore_wait(barrier, ranks - 1 + chips)

    load_w(0).wait()

    @pl.when(me < ranks - 1)
    def _():
        along(0, 1).start()

    @pl.when(me > 0)
    def _():
        along(0, -1).start()

    i0 = lax.broadcasted_iota(jnp.int32, (SPAN, SPAN), 0)
    i1 = lax.broadcasted_iota(jnp.int32, (SPAN, SPAN), 1)
    lower = i0 >= i1
    tril = jnp.where(lower, 1.0, 0.0).astype(F32)
    spread = expander(heads, width)
    spread16 = spread.astype(BF16)
    s_ref[...] = jnp.zeros_like(s_ref)
    l_ref[...] = jnp.ones_like(l_ref)
    for copy in smalls[:3]:
        copy.wait()

    def scan(c, carry):
        at = span_at(c)
        load_x(c).wait()
        load_g(c).start()
        slot = c * SPAN + lax.broadcasted_iota(jnp.int32, (heads, SPAN), 1)
        live = slot < valid
        ld = jnp.where(live, dr_ref[:, at] * (-LOG2E), 0.0)
        run = contract(ld, tril, 1, 1, HIGH)
        runT = contract(tril, ld, 1, 1, HIGH)
        q = jnp.where(live, run - jnp.log2(st_ref[:, at]), 1e30)
        runT_ref[at, :] = runT
        q_ref[:, at] = q
        tail = jnp.exp2(run[:, SPAN - 1 :] - q)
        hi, lo = halves(tail)
        texp = contract(hi, spread16, 0, 0) + contract(lo, spread16, 0, 0)
        weighted = (x_ref[at, :].astype(F32) * texp).astype(BF16)
        fresh = contract(b_ref[at, :], weighted, 0, 0)
        dec = contract(jnp.exp2(runT[SPAN - 8 :, :]), spread, 1, 0, HIGH)[7:8, :]
        before_ref[c] = s_ref[...]
        lead_ref[c] = l_ref[...]
        s_ref[...] = dec * s_ref[...] + fresh
        l_ref[...] = l_ref[...] * dec
        return carry

    lax.fori_loop(0, blocks, scan, 0)
    mine_ref[0:state, :] = s_ref[...].astype(BF16)
    mine_ref[state:, :] = pack_rows(l_ref[0:1, :])

    pair = pltpu.make_async_remote_copy(
        src_ref=mine_ref,
        dst_ref=other_ref,
        send_sem=pair_s.at[0],
        recv_sem=pair_r.at[0],
        device_id={"seq": sibling},
        device_id_type=MESH,
    )
    pair.start()

    def load_ws(i, carry):
        load_w(i).start()
        return carry

    lax.fori_loop(1, shards, load_ws, 0)
    pair.wait()
    cols = pl.ds(pl.multiple_of(core * half, half), half)
    own = mine_ref[:, cols].astype(F32)
    peer = other_ref[:, cols].astype(F32)
    first = jnp.where(core == 0, own, peer)
    second = jnp.where(core == 0, peer, own)
    first_dec = unpack_rows(first[state:, :])
    second_dec = unpack_rows(second[state:, :])
    chip_ref[0:state, :] = (second_dec * first[0:state, :] + second[0:state, :]).astype(BF16)
    chip_ref[state:, :] = pack_rows(first_dec * second_dec)

    def to_chip(j, other):
        return pltpu.make_async_remote_copy(
            src_ref=chip_ref,
            dst_ref=chips_ref.at[j],
            send_sem=chip_s.at[j],
            recv_sem=chip_r.at[j],
            device_id={"seq": other * 2 + core},
            device_id_type=MESH,
        )

    def tell(j, carry):
        @pl.when(chip + j < chips)
        def _():
            to_chip(j, chip + j).start()

        return carry

    lax.fori_loop(1, chips, tell, 0)
    inc_ref[:, cols] = jnp.zeros((state, half), F32)

    def hear(i, carry):
        j = chips - i

        @pl.when(j <= chip)
        def _():
            to_chip(j, chip - j).wait_recv()
            block = chips_ref[j]
            decay = unpack_rows(block[state:, :])
            inc_ref[:, cols] = decay * inc_ref[:, cols] + block[0:state, :].astype(F32)

        return carry

    lax.fori_loop(1, chips, hear, 0)
    swap = pltpu.make_async_remote_copy(
        src_ref=inc_ref.at[:, cols],
        dst_ref=inc_ref.at[:, cols],
        send_sem=pair_s.at[1],
        recv_sem=pair_r.at[1],
        device_id={"seq": sibling},
        device_id_type=MESH,
    )
    swap.start()
    swap.wait()
    inc = inc_ref[...]
    after = unpack_rows(other_ref[state:, :]) * inc + other_ref[0:state, :].astype(F32)
    inc_ref[...] = jnp.where(core == 1, after, inc)

    relay(1)
    smalls[3].wait()
    left = lax.broadcasted_iota(jnp.int32, (SPAN, 128), 1) < (width // heads)
    ones = jnp.ones((8, 128), F32)

    def copies(dest, j, slot):
        c = dest * each + j
        big = pltpu.make_async_remote_copy(
            src_ref=g_ref.at[span_at(c), :],
            dst_ref=got_ref.at[slot, pl.ds(j * SPAN, SPAN), :],
            send_sem=send_sem.at[slot, j],
            recv_sem=recv_sem.at[slot, j],
            device_id={"head": dest},
            device_id_type=MESH,
        )
        small = pltpu.make_async_remote_copy(
            src_ref=ss_buf.at[c],
            dst_ref=ss_ref.at[slot, j],
            send_sem=ssend_sem.at[slot, j],
            recv_sem=srecv_sem.at[slot, j],
            device_id={"head": dest},
            device_id_type=MESH,
        )
        return big, small

    def span(c):
        at = span_at(c)
        load_g(c).wait()
        cb = c_ref[at, :]
        gram = jnp.where(lower, contract(cb, b_ref[at, :], 1, 1), 0.0)
        held = (before_ref[c] + lead_ref[c, 0:1, :] * inc_ref[...]).astype(BF16)
        runT = runT_ref[at, :]
        q = q_ref[:, at]
        hi, lo = halves(jnp.exp2(runT))
        acc = jnp.zeros((SPAN, 128), F32)
        for p in range(width // 128):
            lanes = slice(p * 128, p * 128 + 128)
            xp = x_ref[at, lanes]
            grow = contract(hi, spread16[:, lanes], 1, 0) + contract(lo, spread16[:, lanes], 1, 0)
            carried = contract(cb, held[:, lanes], 1, 0) * grow
            sides = []
            for h in (2 * p, 2 * p + 1):
                m = (
                    gram * jnp.exp2(jnp.minimum(runT[:, h : h + 1] - q[h : h + 1, :], 0.0))
                ).astype(BF16)
                sides.append(jnp.dot(m, xp, preferred_element_type=F32))
            inner = jnp.where(left, sides[0], sides[1])
            z = g_ref[at, lanes].astype(F32)
            skip = jnp.where(left[0:1, :], skip_ref[2 * p], skip_ref[2 * p + 1])
            gated = (inner + carried + skip * xp.astype(F32)) * (
                z * (0.5 * jnp.tanh(0.5 * z) + 0.5)
            )
            acc = acc + gated * gated
            g_ref[at, lanes] = (gated * gain_ref[:, lanes]).astype(BF16)
        ss_buf[c] = contract(ones, acc, 1, 1, HIGH)

    if ranks == 4:
        order = [ranks - 1 - me, lax.rem(me + 2, ranks), me + 1 - 2 * lax.rem(me, 2)]
    else:
        order = [lax.rem(me + k, ranks) for k in range(1, ranks)]
    for index, dest in enumerate(order):
        slot = lax.rem(me - dest + ranks, ranks) - 1

        def one(j, carry, dest=dest, slot=slot):
            span(dest * each + j)
            for copy in copies(dest, j, slot):
                copy.start()
            return carry

        lax.fori_loop(0, each, one, 0)
        if index + 2 < ranks:
            relay(index + 2)

    def mine(j, carry):
        span(me * each + j)
        return carry

    lax.fori_loop(0, each, mine, 0)

    def wait_ws(i, carry):
        load_w(i).wait()
        return carry

    lax.fori_loop(1, shards, wait_ws, 0)
    local = pl.ds(pl.multiple_of(me * share, share), share)

    def own_tile(n, carry):
        lanes = pl.ds(pl.multiple_of(n * TILE, TILE), TILE)
        acc_ref[:, lanes] = jnp.dot(
            g_ref[local, :], w_ref[me, :, lanes], preferred_element_type=F32
        )
        return carry

    lax.fori_loop(0, tiles, own_tile, 0)

    table = near_order(ranks)

    def collect(i):
        r = pick([row[i] for row in table], me)
        slot = lax.rem(r - me + ranks, ranks) - 1

        def pass_on(j, carry):
            landed(r, j).wait_recv()
            across(r, j, core).start()
            return carry

        def wait_across(j, carry):
            across(r, j, 1 - core).wait_recv()
            return carry

        def wait_got(j, carry):
            for copy in copies(r, j, slot):
                copy.wait_recv()
            return carry

        lax.fori_loop(1, chips, pass_on, 0)
        lax.fori_loop(0, chips, wait_across, 0)
        lax.fori_loop(0, each, wait_got, 0)
        return r, slot

    for i in range(ranks - 2):
        r, slot = collect(i)

        def more(n, carry, r=r, slot=slot):
            lanes = pl.ds(pl.multiple_of(n * TILE, TILE), TILE)
            acc_ref[:, lanes] += jnp.dot(
                got_ref[slot], w_ref[r, :, lanes], preferred_element_type=F32
            )
            return carry

        lax.fori_loop(0, tiles, more, 0)

    r, slot = collect(ranks - 2)
    unit = jnp.where(lax.broadcasted_iota(jnp.int32, (8, 128), 0) == 0, 1.0, 0.0).astype(F32)
    scales = []
    for j in range(each):
        total = ss_buf[me * each + j]
        for k in range(ranks - 1):
            total = total + ss_ref[k, j]
        column = contract(total, unit, 0, 0, HIGH) * (1.0 / (width * ranks))
        token = (
            me * share + j * SPAN + lax.broadcasted_iota(jnp.int32, (SPAN, 128), 0)
        )
        scales.append(jnp.where(token < valid, lax.rsqrt(column + 1e-05), 0.0))
    scale = jnp.concatenate(scales, axis=0)

    def put(n):
        lanes = pl.ds(pl.multiple_of(n * TILE, TILE), TILE)
        return pltpu.make_async_copy(res_ref.at[:, lanes], out_hbm.at[:, lanes], out_sem.at[n])

    wide = jnp.concatenate([scale] * (TILE // 128), axis=1)

    def final(n, carry):
        lanes = pl.ds(pl.multiple_of(n * TILE, TILE), TILE)
        part = jnp.dot(got_ref[slot], w_ref[r, :, lanes], preferred_element_type=F32)
        res_ref[:, lanes] = ((acc_ref[:, lanes] + part) * wide).astype(BF16)
        put(n).start()
        return carry

    lax.fori_loop(0, tiles, final, 0)

    for k in range(ranks - 1):
        for step in (1, -1):
            source = me - step * k
            last = me == (ranks - 1 if step > 0 else 0)

            @pl.when((source >= 0) & (source < ranks) & jnp.logical_not(last))
            def _(k=k, step=step):
                along(k, step).wait_send()

    for i in range(ranks - 1):
        r = pick([row[i] for row in table], me)

        def sent_plane(j, carry, r=r):
            plane(r, j).wait_send()
            return carry

        def sent_across(j, carry, r=r):
            across(r, j, core).wait_send()
            return carry

        lax.fori_loop(1, chips, sent_plane, 0)
        lax.fori_loop(0, chips, sent_across, 0)

    def told(j, carry):
        @pl.when(chip + j < chips)
        def _():
            to_chip(j, chip + j).wait_send()

        return carry

    lax.fori_loop(1, chips, told, 0)
    for dest in order:
        slot = lax.rem(me - dest + ranks, ranks) - 1

        def sent(j, carry, dest=dest, slot=slot):
            for copy in copies(dest, j, slot):
                copy.wait_send()
            return carry

        lax.fori_loop(0, each, sent, 0)

    def wait_put(n, carry):
        put(n).wait()
        return carry

    lax.fori_loop(0, tiles, wait_put, 0)


def body(
    ranks,
    shards,
    values,
    gates,
    b_proj,
    c_proj,
    step_size,
    decay_rate,
    skip_gain,
    norm_gain,
    readout,
    span_counts,
    remaining_count,
):
    length, width = values.shape
    heads = step_size.shape[0]
    state = b_proj.shape[1]
    depth = readout.shape[1]
    blocks = length // SPAN
    share = length // ranks
    each = blocks // ranks
    chips = shards // 2
    sds = jax.ShapeDtypeStruct
    smem = pl.BlockSpec(memory_space=pltpu.SMEM)
    hbm = pl.BlockSpec(memory_space=pl.ANY)
    dma = pltpu.SemaphoreType.DMA
    return pl.pallas_call(
        functools.partial(layer_kernel, ranks, shards),
        out_shape=sds((share, depth), BF16),
        in_specs=[smem, smem, smem, pl.BlockSpec(memory_space=VMEM)] + [hbm] * 7,
        out_specs=hbm,
        scratch_shapes=[
            VMEM((length, width), BF16),
            VMEM((length, width), BF16),
            VMEM((length, state), BF16),
            VMEM((length, state), BF16),
            VMEM((heads, length), F32),
            VMEM((heads, length), F32),
            VMEM((length, heads), F32),
            VMEM((heads, length), F32),
            VMEM((blocks, state, width), F32),
            VMEM((blocks, 8, width), F32),
            VMEM((state, width), F32),
            VMEM((8, width), F32),
            VMEM((state + 16, width), BF16),
            VMEM((state + 16, width), BF16),
            VMEM((state + 16, width // 2), BF16),
            VMEM((chips, state + 16, width // 2), BF16),
            VMEM((state, width), F32),
            VMEM((ranks, width, depth), BF16),
            VMEM((ranks - 1, share, width), BF16),
            VMEM((blocks, 8, SPAN), F32),
            VMEM((ranks - 1, each, 8, SPAN), F32),
            VMEM((share, depth), F32),
            VMEM((share, depth), BF16),
            dma((blocks,)),
            dma((blocks,)),
            dma((4,)),
            dma((shards,)),
            dma((ranks - 1,)),
            dma((ranks - 1,)),
            dma((ranks - 1,)),
            dma((ranks - 1,)),
            dma((ranks - 1, chips)),
            dma((ranks - 1, chips)),
            dma((ranks - 1, chips)),
            dma((ranks - 1, chips)),
            dma((2,)),
            dma((2,)),
            dma((chips,)),
            dma((chips,)),
            dma((ranks - 1, each)),
            dma((ranks - 1, each)),
            dma((ranks - 1, each)),
            dma((ranks - 1, each)),
            dma((depth // TILE,)),
        ],
        compiler_params=pltpu.CompilerParams(
            vmem_limit_bytes=LIMIT, collective_id=0, has_side_effects=True
        ),
        cost_estimate=pl.CostEstimate(
            flops=10**11, bytes_accessed=20 * 10**6, transcendentals=0
        ),
        name="layer",
    )(
        span_counts,
        remaining_count,
        skip_gain,
        norm_gain[None, :],
        values,
        gates,
        b_proj,
        c_proj,
        step_size,
        decay_rate,
        readout,
    )


def solution(mesh):
    return jax.shard_map(
        functools.partial(body, mesh.shape["head"], mesh.shape["seq"]),
        mesh=mesh,
        in_specs=(
            P("seq", "head"),
            P("seq", "head"),
            P("seq", None),
            P("seq", None),
            P("head", "seq"),
            P("head", "seq"),
            P("head"),
            P("head"),
            P("head", None),
            P("seq"),
            P("seq"),
        ),
        out_specs=P(("seq", "head"), None),
        check_vma=False,
    )
```

```python
import functools
import math

import jax
import jax.numpy as jnp
from jax import lax
from jax.experimental import pallas as pl
from jax.experimental.pallas import tpu as pltpu
from jax.sharding import PartitionSpec as P

SPAN = 256
LOG2E = math.log2(math.e)
F32 = jnp.float32
BF16 = jnp.bfloat16
HIGH = lax.Precision.HIGHEST
MESH = pl.DeviceIdType.MESH
VMEM = pltpu.VMEM
LIMIT = 63 * 1024 * 1024
TILE = 256


def contract(a, b, da, db, precision=None):
    return lax.dot_general(
        a, b, (((da,), (db,)), ((), ())), precision=precision, preferred_element_type=F32
    )


def expander(heads, width):
    size = width // heads
    col = lax.broadcasted_iota(jnp.int32, (heads, width), 1) // size
    row = lax.broadcasted_iota(jnp.int32, (heads, width), 0)
    return jnp.where(col == row, 1.0, 0.0).astype(F32)


def halves(a):
    hi = a.astype(BF16)
    return hi, (a - hi.astype(F32)).astype(BF16)


def pack_rows(total):
    total = jnp.broadcast_to(total, (16, total.shape[1]))
    hi, mid = halves(total)
    low = (total - hi.astype(F32) - mid.astype(F32)).astype(BF16)
    row = lax.broadcasted_iota(jnp.int32, total.shape, 0)
    parts = jnp.where(row == 0, hi.astype(F32), jnp.where(row == 1, mid.astype(F32), low.astype(F32)))
    return jnp.where(row < 3, parts, 0.0).astype(BF16)


def unpack_rows(rows):
    rows = rows.astype(F32)
    return rows[0:1, :] + rows[1:2, :] + rows[2:3, :]


def pick(table, index):
    total = jnp.int32(0)
    for i, value in enumerate(table):
        total = total + jnp.where(index == i, jnp.int32(value), jnp.int32(0))
    return total


def near_order(ranks):
    return [sorted((r for r in range(ranks) if r != h), key=lambda r: (abs(r - h), r)) for h in range(ranks)]


def weight_moves(ranks):
    if ranks != 4:
        return [(r, r, t, 0) for r in range(ranks) for t in range(ranks) if t != r]
    right = [(0, 0, 2, 0), (0, 0, 1, 0), (2, 2, 3, 0), (1, 1, 2, 0), (0, 2, 3, 2), (1, 2, 3, 3)]
    return right + [(3 - r, 3 - a, 3 - b, phase) for r, a, b, phase in right]


def late_order(ranks):
    if ranks == 4:
        return [[1, 3, 2], [0, 3, 2], [3, 0, 1], [2, 0, 1]]
    return near_order(ranks)


def layer_kernel(
    ranks,
    shards,
    count_ref,
    remain_ref,
    skip_ref,
    gain_ref,
    x_hbm,
    g_hbm,
    b_hbm,
    c_hbm,
    st_hbm,
    dr_hbm,
    w_hbm,
    out_hbm,
    x_ref,
    g_ref,
    b_ref,
    c_ref,
    st_ref,
    dr_ref,
    runT_ref,
    q_ref,
    before_ref,
    lead_ref,
    s_ref,
    l_ref,
    mine_ref,
    other_ref,
    chip_ref,
    chips_ref,
    inc_ref,
    w_ref,
    got_ref,
    ss_buf,
    ss_ref,
    acc_ref,
    res_ref,
    x_sem,
    g_sem,
    in_sem,
    w_sem,
    along_s,
    along_r,
    plane_s,
    plane_r,
    sib_s,
    sib_r,
    pair_s,
    pair_r,
    chip_s,
    chip_r,
    send_sem,
    recv_sem,
    ssend_sem,
    srecv_sem,
    out_sem,
):
    heads, length = q_ref.shape
    width = x_ref.shape[1]
    blocks = length // SPAN
    each = blocks // ranks
    share = length // ranks
    state = s_ref.shape[0]
    depth = res_ref.shape[1]
    rows = width // shards
    chips = shards // 2
    half = width // 2
    tiles = depth // TILE
    me = lax.axis_index("head")
    place = lax.axis_index("seq")
    core = lax.rem(place, 2)
    chip = lax.div(place, 2)
    sibling = place + 1 - 2 * core
    valid = (count_ref[0] - 1) * SPAN + remain_ref[0]

    def span_at(c):
        return pl.ds(pl.multiple_of(c * SPAN, SPAN), SPAN)

    def slice_at(owner):
        return pl.ds(pl.multiple_of(owner * rows, rows), rows)

    def load_w(i):
        owner = lax.rem(place + i, shards)
        return pltpu.make_async_copy(
            w_hbm.at[slice_at(owner), :], w_ref.at[me, slice_at(owner), :], w_sem.at[i]
        )

    def load_x(c):
        return pltpu.make_async_copy(x_hbm.at[span_at(c), :], x_ref.at[span_at(c), :], x_sem.at[c])

    def load_g(c):
        return pltpu.make_async_copy(g_hbm.at[span_at(c), :], g_ref.at[span_at(c), :], g_sem.at[c])

    smalls = [
        pltpu.make_async_copy(src, dst, in_sem.at[i])
        for i, (src, dst) in enumerate(
            ((st_hbm, st_ref), (dr_hbm, dr_ref), (b_hbm, b_ref), (c_hbm, c_ref))
        )
    ]

    moves = weight_moves(ranks)

    def along(owner, dest):
        return pltpu.make_async_remote_copy(
            src_ref=w_ref.at[owner, slice_at(place), :],
            dst_ref=w_ref.at[owner, slice_at(place), :],
            send_sem=along_s.at[owner, dest],
            recv_sem=along_r.at[owner],
            device_id={"head": dest},
            device_id_type=MESH,
        )

    def move(now):
        for h in range(ranks):
            mine = [(r, b) for r, a, b, phase in moves if a == h and phase == now]
            if mine:

                @pl.when(me == h)
                def _(h=h, mine=mine):
                    for r, b in mine:
                        if r != h:
                            along(r, b).wait_recv()
                        along(r, b).start()

    def spread_out(early):
        for h in range(ranks):
            relayed = [r for r, a, b, phase in moves if a == h and r != h]
            outer = ranks == 4 and h in (0, ranks - 1)
            owners = near_order(ranks)[h]
            if outer:
                owners = owners[:1] if early else owners[1:]
            elif not early:
                owners = []
            if owners:

                @pl.when(me == h)
                def _(h=h, relayed=relayed, owners=owners):
                    for r in owners:
                        if r not in relayed:
                            along(r, r).wait_recv()
                        spread_plane(jnp.int32(r))

    square = chips == 4
    direct = (1, 2) if square else tuple(range(1, chips))

    def chip_to(j):
        if square:
            return (chip, chip + 1 - 2 * lax.rem(chip, 2), lax.rem(chip + 2, 4), 3 - chip)[j]
        return lax.rem(chip + j, chips)

    def chip_from(j):
        return chip_to(j) if square else lax.rem(chip - j + chips, chips)

    def over_chips(low, one):
        if square:
            for j in range(low, chips):
                one(j)
        else:

            def step(j, carry):
                one(j)
                return carry

            lax.fori_loop(low, chips, step, 0)

    def plane(r, j):
        slot = lax.rem(r - me + ranks, ranks) - 1
        dest = chip_to(j) * 2 + core
        return pltpu.make_async_remote_copy(
            src_ref=w_ref.at[r, slice_at(place), :],
            dst_ref=w_ref.at[r, slice_at(place), :],
            send_sem=plane_s.at[slot, j],
            recv_sem=plane_r.at[slot, j],
            device_id={"seq": dest},
            device_id_type=MESH,
        )

    def landed(r, j):
        slot = lax.rem(r - me + ranks, ranks) - 1
        owner = chip_from(j) * 2 + core
        return pltpu.make_async_remote_copy(
            src_ref=w_ref.at[r, slice_at(owner), :],
            dst_ref=w_ref.at[r, slice_at(owner), :],
            send_sem=plane_s.at[slot, j],
            recv_sem=plane_r.at[slot, j],
            device_id={"seq": owner},
            device_id_type=MESH,
        )

    def corner(r, part, dest, owner):
        slot = lax.rem(r - me + ranks, ranks) - 1
        low = rows // 32 * 16
        at = pl.ds(
            pl.multiple_of((owner * 2 + core) * rows + (low if part else 0), 16),
            rows - low if part else low,
        )
        return pltpu.make_async_remote_copy(
            src_ref=w_ref.at[r, at, :],
            dst_ref=w_ref.at[r, at, :],
            send_sem=plane_s.at[slot, 3 * part],
            recv_sem=plane_r.at[slot, 3 * part],
            device_id={"seq": dest * 2 + core},
            device_id_type=MESH,
        )

    def turn(r, part):
        return corner(r, part, chip_to(2 - part), chip_to(1 + part))

    def turned(r, part):
        return corner(r, part, chip_to(2 - part), chip_to(3))

    def across(r, j, of_core):
        slot = lax.rem(r - me + ranks, ranks) - 1
        owner = chip_from(j) * 2 + of_core
        return pltpu.make_async_remote_copy(
            src_ref=w_ref.at[r, slice_at(owner), :],
            dst_ref=w_ref.at[r, slice_at(owner), :],
            send_sem=sib_s.at[slot, j],
            recv_sem=sib_r.at[slot, j],
            device_id={"seq": sibling},
            device_id_type=MESH,
        )

    def spread_plane(r):
        across(r, 0, core).start()
        if square:
            for j in direct:
                plane(r, j).start()
        else:
            over_chips(1, lambda j: plane(r, j).start())

    load_w(0).start()
    for copy in smalls[:3]:
        copy.start()

    def load_xs(c, carry):
        load_x(c).start()
        return carry

    lax.fori_loop(0, blocks, load_xs, 0)
    smalls[3].start()

    barrier = pltpu.get_barrier_semaphore()

    def greet(k, carry):
        pl.semaphore_signal(
            barrier, inc=1, device_id={"head": lax.rem(me + k, ranks)}, device_id_type=MESH
        )
        return carry

    def greet_plane(j):
        dest = chip_to(j) * 2 + core
        pl.semaphore_signal(barrier, inc=1, device_id={"seq": dest}, device_id_type=MESH)

    lax.fori_loop(1, ranks, greet, 0)
    over_chips(1, greet_plane)
    pl.semaphore_signal(barrier, inc=1, device_id={"seq": sibling}, device_id_type=MESH)
    pl.semaphore_wait(barrier, ranks - 1 + chips)

    load_w(0).wait()

    move(0)

    i0 = lax.broadcasted_iota(jnp.int32, (SPAN, SPAN), 0)
    i1 = lax.broadcasted_iota(jnp.int32, (SPAN, SPAN), 1)
    lower = i0 >= i1
    tril = jnp.where(lower, 1.0, 0.0).astype(F32)
    spread = expander(heads, width)
    spread16 = spread.astype(BF16)
    s_ref[...] = jnp.zeros_like(s_ref)
    l_ref[...] = jnp.ones_like(l_ref)
    for copy in smalls[:3]:
        copy.wait()

    def scan(c, carry):
        at = span_at(c)
        load_x(c).wait()
        load_g(c).start()
        slot = c * SPAN + lax.broadcasted_iota(jnp.int32, (heads, SPAN), 1)
        live = slot < valid
        ld = jnp.where(live, dr_ref[:, at] * (-LOG2E), 0.0)
        run = contract(ld, tril, 1, 1, HIGH)
        runT = contract(tril, ld, 1, 1, HIGH)
        q = jnp.where(live, run - jnp.log2(st_ref[:, at]), 1e30)
        runT_ref[at, :] = runT
        q_ref[:, at] = q
        tail = jnp.exp2(run[:, SPAN - 1 :] - q)
        hi, lo = halves(tail)
        texp = contract(hi, spread16, 0, 0) + contract(lo, spread16, 0, 0)
        weighted = (x_ref[at, :].astype(F32) * texp).astype(BF16)
        fresh = contract(b_ref[at, :], weighted, 0, 0)
        dec = contract(jnp.exp2(runT[SPAN - 8 :, :]), spread, 1, 0, HIGH)[7:8, :]
        before_ref[c] = s_ref[...]
        lead_ref[c] = l_ref[...]
        s_ref[...] = dec * s_ref[...] + fresh
        l_ref[...] = l_ref[...] * dec
        return carry

    lax.fori_loop(0, blocks, scan, 0)
    move(1)
    mine_ref[0:state, :] = s_ref[...].astype(BF16)
    mine_ref[state:, :] = pack_rows(l_ref[0:1, :])

    pair = pltpu.make_async_remote_copy(
        src_ref=mine_ref,
        dst_ref=other_ref,
        send_sem=pair_s.at[0],
        recv_sem=pair_r.at[0],
        device_id={"seq": sibling},
        device_id_type=MESH,
    )
    pair.start()

    def load_ws(i, carry):
        load_w(i).start()
        return carry

    lax.fori_loop(1, shards, load_ws, 0)
    pair.wait()
    cols = pl.ds(pl.multiple_of(core * half, half), half)
    own = mine_ref[:, cols].astype(F32)
    peer = other_ref[:, cols].astype(F32)
    first = jnp.where(core == 0, own, peer)
    second = jnp.where(core == 0, peer, own)
    first_dec = unpack_rows(first[state:, :])
    second_dec = unpack_rows(second[state:, :])
    chip_ref[0:state, :] = (second_dec * first[0:state, :] + second[0:state, :]).astype(BF16)
    chip_ref[state:, :] = pack_rows(first_dec * second_dec)

    def to_chip(j, other):
        return pltpu.make_async_remote_copy(
            src_ref=chip_ref,
            dst_ref=chips_ref.at[j],
            send_sem=chip_s.at[j],
            recv_sem=chip_r.at[j],
            device_id={"seq": other * 2 + core},
            device_id_type=MESH,
        )

    def tell(j, carry):
        @pl.when(chip + j < chips)
        def _():
            to_chip(j, chip + j).start()

        return carry

    lax.fori_loop(1, chips, tell, 0)
    move(2)
    inc_ref[:, cols] = jnp.zeros((state, half), F32)

    def hear(i, carry):
        j = chips - i

        @pl.when(j <= chip)
        def _():
            to_chip(j, chip - j).wait_recv()
            block = chips_ref[j]
            decay = unpack_rows(block[state:, :])
            inc_ref[:, cols] = decay * inc_ref[:, cols] + block[0:state, :].astype(F32)

        return carry

    lax.fori_loop(1, chips, hear, 0)
    swap = pltpu.make_async_remote_copy(
        src_ref=inc_ref.at[:, cols],
        dst_ref=inc_ref.at[:, cols],
        send_sem=pair_s.at[1],
        recv_sem=pair_r.at[1],
        device_id={"seq": sibling},
        device_id_type=MESH,
    )
    swap.start()
    swap.wait()
    inc = inc_ref[...]
    after = unpack_rows(other_ref[state:, :]) * inc + other_ref[0:state, :].astype(F32)
    inc_ref[...] = jnp.where(core == 1, after, inc)

    smalls[3].wait()
    left = lax.broadcasted_iota(jnp.int32, (SPAN, 128), 1) < (width // heads)
    ones = jnp.ones((8, 128), F32)

    def copies(dest, j, slot):
        c = dest * each + j
        big = pltpu.make_async_remote_copy(
            src_ref=g_ref.at[span_at(c), :],
            dst_ref=got_ref.at[slot, pl.ds(j * SPAN, SPAN), :],
            send_sem=send_sem.at[slot, j],
            recv_sem=recv_sem.at[slot, j],
            device_id={"head": dest},
            device_id_type=MESH,
        )
        small = pltpu.make_async_remote_copy(
            src_ref=ss_buf.at[c],
            dst_ref=ss_ref.at[slot, j],
            send_sem=ssend_sem.at[slot, j],
            recv_sem=srecv_sem.at[slot, j],
            device_id={"head": dest},
            device_id_type=MESH,
        )
        return big, small

    def span(c):
        at = span_at(c)
        load_g(c).wait()
        cb = c_ref[at, :]
        gram = jnp.where(lower, contract(cb, b_ref[at, :], 1, 1), 0.0)
        held = (before_ref[c] + lead_ref[c, 0:1, :] * inc_ref[...]).astype(BF16)
        runT = runT_ref[at, :]
        q = q_ref[:, at]
        hi, lo = halves(jnp.exp2(runT))
        acc = jnp.zeros((SPAN, 128), F32)
        for p in range(width // 128):
            lanes = slice(p * 128, p * 128 + 128)
            xp = x_ref[at, lanes]
            grow = contract(hi, spread16[:, lanes], 1, 0) + contract(lo, spread16[:, lanes], 1, 0)
            carried = contract(cb, held[:, lanes], 1, 0) * grow
            sides = []
            for h in (2 * p, 2 * p + 1):
                m = (
                    gram * jnp.exp2(jnp.minimum(runT[:, h : h + 1] - q[h : h + 1, :], 0.0))
                ).astype(BF16)
                sides.append(jnp.dot(m, xp, preferred_element_type=F32))
            inner = jnp.where(left, sides[0], sides[1])
            z = g_ref[at, lanes].astype(F32)
            skip = jnp.where(left[0:1, :], skip_ref[2 * p], skip_ref[2 * p + 1])
            gated = (inner + carried + skip * xp.astype(F32)) * (
                z * (0.5 * jnp.tanh(0.5 * z) + 0.5)
            )
            acc = acc + gated * gated
            g_ref[at, lanes] = (gated * gain_ref[:, lanes]).astype(BF16)
        ss_buf[c] = contract(ones, acc, 1, 1, HIGH)

    if ranks == 4:
        order = [ranks - 1 - me, lax.rem(me + 2, ranks), me + 1 - 2 * lax.rem(me, 2)]
    else:
        order = [lax.rem(me + k, ranks) for k in range(1, ranks)]
    for index, dest in enumerate(order):
        slot = lax.rem(me - dest + ranks, ranks) - 1

        def one(j, carry, dest=dest, slot=slot):
            span(dest * each + j)
            for copy in copies(dest, j, slot):
                copy.start()
            return carry

        lax.fori_loop(0, each, one, 0)
        if index == 0:
            move(3)
            spread_out(True)

    def mine(j, carry):
        span(me * each + j)
        return carry

    lax.fori_loop(0, each, mine, 0)

    def wait_ws(i, carry):
        load_w(i).wait()
        return carry

    lax.fori_loop(1, shards, wait_ws, 0)
    local = pl.ds(pl.multiple_of(me * share, share), share)

    def own_tile(n, carry):
        lanes = pl.ds(pl.multiple_of(n * TILE, TILE), TILE)
        acc_ref[:, lanes] = jnp.dot(
            g_ref[local, :], w_ref[me, :, lanes], preferred_element_type=F32
        )
        return carry

    lax.fori_loop(0, tiles, own_tile, 0)

    near = near_order(ranks)
    late = late_order(ranks)

    def source_of(table, i):
        return pick([row[i] for row in table], me)

    def pass_direct(i):
        r = source_of(near, i)
        if square:
            for j in direct:
                landed(r, j).wait_recv()
                turn(r, j - 1).start()
                across(r, j, core).start()
        else:

            def one(j):
                landed(r, j).wait_recv()
                across(r, j, core).start()

            over_chips(1, one)

    def pass_corner(i):
        r = source_of(near, i)
        if square:
            for part in (0, 1):
                turned(r, part).wait_recv()
            across(r, 3, core).start()
        over_chips(0, lambda j: across(r, j, 1 - core).wait_recv())

    pass_direct(0)
    spread_out(False)
    for i in range(1, ranks - 1):
        pass_direct(i)
        pass_corner(i - 1)
    pass_corner(ranks - 2)

    def take(i):
        r = source_of(late, i)
        return r, lax.rem(r - me + ranks, ranks) - 1

    def receive(r, slot, j):
        for copy in copies(r, j, slot):
            copy.wait_recv()

    for i in range(ranks - 2):
        r, slot = take(i)
        for j in range(each):
            receive(r, slot, j)

        def more(n, carry, r=r, slot=slot):
            lanes = pl.ds(pl.multiple_of(n * TILE, TILE), TILE)
            acc_ref[:, lanes] += jnp.dot(
                got_ref[slot], w_ref[r, :, lanes], preferred_element_type=F32
            )
            return carry

        lax.fori_loop(0, tiles, more, 0)

    r, slot = take(ranks - 2)
    unit = jnp.where(lax.broadcasted_iota(jnp.int32, (8, 128), 0) == 0, 1.0, 0.0).astype(F32)

    def put(n, j):
        lanes = pl.ds(pl.multiple_of(n * TILE, TILE), TILE)
        at = pl.ds(j * SPAN, SPAN)
        return pltpu.make_async_copy(
            res_ref.at[at, lanes], out_hbm.at[at, lanes], out_sem.at[n, j]
        )

    for j in range(each):
        receive(r, slot, j)
        total = ss_buf[me * each + j]
        for k in range(ranks - 1):
            total = total + ss_ref[k, j]
        column = contract(total, unit, 0, 0, HIGH) * (1.0 / (width * ranks))
        token = me * share + j * SPAN + lax.broadcasted_iota(jnp.int32, (SPAN, 128), 0)
        scale = jnp.where(token < valid, lax.rsqrt(column + 1e-05), 0.0)
        wide = jnp.concatenate([scale] * (TILE // 128), axis=1)
        at = pl.ds(j * SPAN, SPAN)

        def final(n, carry, j=j, at=at, wide=wide):
            lanes = pl.ds(pl.multiple_of(n * TILE, TILE), TILE)
            part = jnp.dot(got_ref[slot, at, :], w_ref[r, :, lanes], preferred_element_type=F32)
            res_ref[at, lanes] = ((acc_ref[at, lanes] + part) * wide).astype(BF16)
            put(n, j).start()
            return carry

        lax.fori_loop(0, tiles, final, 0)

    for h in range(ranks):

        @pl.when(me == h)
        def _(h=h):
            for r, a, b, phase in moves:
                if a == h:
                    along(r, b).wait_send()

    for i in range(ranks - 1):
        r = source_of(near, i)
        if square:
            for j in direct:
                plane(r, j).wait_send()
                turn(r, j - 1).wait_send()
        else:
            over_chips(1, lambda j: plane(r, j).wait_send())
        over_chips(0, lambda j: across(r, j, core).wait_send())

    def told(j, carry):
        @pl.when(chip + j < chips)
        def _():
            to_chip(j, chip + j).wait_send()

        return carry

    lax.fori_loop(1, chips, told, 0)
    for dest in order:
        slot = lax.rem(me - dest + ranks, ranks) - 1

        def sent(j, carry, dest=dest, slot=slot):
            for copy in copies(dest, j, slot):
                copy.wait_send()
            return carry

        lax.fori_loop(0, each, sent, 0)

    def wait_put(n, carry):
        for j in range(each):
            put(n, j).wait()
        return carry

    lax.fori_loop(0, tiles, wait_put, 0)


def body(
    ranks,
    shards,
    values,
    gates,
    b_proj,
    c_proj,
    step_size,
    decay_rate,
    skip_gain,
    norm_gain,
    readout,
    span_counts,
    remaining_count,
):
    length, width = values.shape
    heads = step_size.shape[0]
    state = b_proj.shape[1]
    depth = readout.shape[1]
    blocks = length // SPAN
    share = length // ranks
    each = blocks // ranks
    chips = shards // 2
    sds = jax.ShapeDtypeStruct
    smem = pl.BlockSpec(memory_space=pltpu.SMEM)
    hbm = pl.BlockSpec(memory_space=pl.ANY)
    dma = pltpu.SemaphoreType.DMA
    return pl.pallas_call(
        functools.partial(layer_kernel, ranks, shards),
        out_shape=sds((share, depth), BF16),
        in_specs=[smem, smem, smem, pl.BlockSpec(memory_space=VMEM)] + [hbm] * 7,
        out_specs=hbm,
        scratch_shapes=[
            VMEM((length, width), BF16),
            VMEM((length, width), BF16),
            VMEM((length, state), BF16),
            VMEM((length, state), BF16),
            VMEM((heads, length), F32),
            VMEM((heads, length), F32),
            VMEM((length, heads), F32),
            VMEM((heads, length), F32),
            VMEM((blocks, state, width), F32),
            VMEM((blocks, 8, width), F32),
            VMEM((state, width), F32),
            VMEM((8, width), F32),
            VMEM((state + 16, width), BF16),
            VMEM((state + 16, width), BF16),
            VMEM((state + 16, width // 2), BF16),
            VMEM((chips, state + 16, width // 2), BF16),
            VMEM((state, width), F32),
            VMEM((ranks, width, depth), BF16),
            VMEM((ranks - 1, share, width), BF16),
            VMEM((blocks, 8, SPAN), F32),
            VMEM((ranks - 1, each, 8, SPAN), F32),
            VMEM((share, depth), F32),
            VMEM((share, depth), BF16),
            dma((blocks,)),
            dma((blocks,)),
            dma((4,)),
            dma((shards,)),
            dma((ranks, ranks)),
            dma((ranks,)),
            dma((ranks - 1, chips)),
            dma((ranks - 1, chips)),
            dma((ranks - 1, chips)),
            dma((ranks - 1, chips)),
            dma((2,)),
            dma((2,)),
            dma((chips,)),
            dma((chips,)),
            dma((ranks - 1, each)),
            dma((ranks - 1, each)),
            dma((ranks - 1, each)),
            dma((ranks - 1, each)),
            dma((depth // TILE, each)),
        ],
        compiler_params=pltpu.CompilerParams(
            vmem_limit_bytes=LIMIT, collective_id=0, has_side_effects=True
        ),
        cost_estimate=pl.CostEstimate(
            flops=10**11, bytes_accessed=20 * 10**6, transcendentals=0
        ),
        name="layer",
    )(
        span_counts,
        remaining_count,
        skip_gain,
        norm_gain[None, :],
        values,
        gates,
        b_proj,
        c_proj,
        step_size,
        decay_rate,
        readout,
    )


def solution(mesh):
    return jax.shard_map(
        functools.partial(body, mesh.shape["head"], mesh.shape["seq"]),
        mesh=mesh,
        in_specs=(
            P("seq", "head"),
            P("seq", "head"),
            P("seq", None),
            P("seq", None),
            P("head", "seq"),
            P("head", "seq"),
            P("head"),
            P("head"),
            P("head", None),
            P("seq"),
            P("seq"),
        ),
        out_specs=P(("seq", "head"), None),
        check_vma=False,
    )
```

```python
import functools
import math

import jax
import jax.numpy as jnp
from jax import lax
from jax.experimental import pallas as pl
from jax.experimental.pallas import tpu as pltpu
from jax.sharding import PartitionSpec as P

SPAN = 256
LOG2E = math.log2(math.e)
F32 = jnp.float32
BF16 = jnp.bfloat16
HIGH = lax.Precision.HIGHEST
MESH = pl.DeviceIdType.MESH
VMEM = pltpu.VMEM
LIMIT = 63 * 1024 * 1024
TILE = 256


def contract(a, b, da, db, precision=None):
    return lax.dot_general(
        a, b, (((da,), (db,)), ((), ())), precision=precision, preferred_element_type=F32
    )


def expander(heads, width):
    size = width // heads
    col = lax.broadcasted_iota(jnp.int32, (heads, width), 1) // size
    row = lax.broadcasted_iota(jnp.int32, (heads, width), 0)
    return jnp.where(col == row, 1.0, 0.0).astype(F32)


def halves(a):
    hi = a.astype(BF16)
    return hi, (a - hi.astype(F32)).astype(BF16)


def pack_rows(total):
    total = jnp.broadcast_to(total, (16, total.shape[1]))
    hi, mid = halves(total)
    low = (total - hi.astype(F32) - mid.astype(F32)).astype(BF16)
    row = lax.broadcasted_iota(jnp.int32, total.shape, 0)
    parts = jnp.where(row == 0, hi.astype(F32), jnp.where(row == 1, mid.astype(F32), low.astype(F32)))
    return jnp.where(row < 3, parts, 0.0).astype(BF16)


def unpack_rows(rows):
    rows = rows.astype(F32)
    return rows[0:1, :] + rows[1:2, :] + rows[2:3, :]


def pick(table, index):
    total = jnp.int32(0)
    for i, value in enumerate(table):
        total = total + jnp.where(index == i, jnp.int32(value), jnp.int32(0))
    return total


def near_order(ranks):
    return [sorted((r for r in range(ranks) if r != h), key=lambda r: (abs(r - h), r)) for h in range(ranks)]


def weight_moves(ranks):
    if ranks != 4:
        return [
            (r, r, t, part, 0) for part in (0, 1) for r in range(ranks) for t in range(ranks) if t != r
        ]
    right = [(0, 0, 2, 0, 0), (0, 0, 2, 1, 0), (0, 0, 1, 0, 0), (0, 0, 1, 1, 0)]
    right += [(2, 2, 3, 0, 0), (2, 2, 3, 1, 0), (1, 1, 2, 0, 0), (1, 1, 2, 1, 0)]
    right += [(0, 2, 3, 0, 1), (0, 2, 3, 1, 2), (1, 2, 3, 0, 3), (1, 2, 3, 1, 3)]
    return right + [(3 - r, 3 - a, 3 - b, part, phase) for r, a, b, part, phase in right]


def late_order(ranks):
    if ranks == 4:
        return [[1, 3, 2], [0, 3, 2], [3, 0, 1], [2, 0, 1]]
    return near_order(ranks)


def layer_kernel(
    ranks,
    shards,
    count_ref,
    remain_ref,
    skip_ref,
    gain_ref,
    x_hbm,
    g_hbm,
    b_hbm,
    c_hbm,
    st_hbm,
    dr_hbm,
    w_hbm,
    out_hbm,
    x_ref,
    g_ref,
    b_ref,
    c_ref,
    st_ref,
    dr_ref,
    runT_ref,
    q_ref,
    before_ref,
    lead_ref,
    s_ref,
    l_ref,
    mine_ref,
    other_ref,
    chip_ref,
    chips_ref,
    inc_ref,
    w_ref,
    got_ref,
    ss_buf,
    ss_ref,
    acc_ref,
    res_ref,
    x_sem,
    g_sem,
    in_sem,
    w_sem,
    along_s,
    along_r,
    plane_s,
    plane_r,
    sib_s,
    sib_r,
    pair_s,
    pair_r,
    chip_s,
    chip_r,
    send_sem,
    recv_sem,
    ssend_sem,
    srecv_sem,
    out_sem,
):
    heads, length = q_ref.shape
    width = x_ref.shape[1]
    blocks = length // SPAN
    each = blocks // ranks
    share = length // ranks
    state = s_ref.shape[0]
    depth = res_ref.shape[1]
    rows = width // shards
    chips = shards // 2
    half = width // 2
    tiles = depth // TILE
    me = lax.axis_index("head")
    place = lax.axis_index("seq")
    core = lax.rem(place, 2)
    chip = lax.div(place, 2)
    sibling = place + 1 - 2 * core
    valid = (count_ref[0] - 1) * SPAN + remain_ref[0]

    def span_at(c):
        return pl.ds(pl.multiple_of(c * SPAN, SPAN), SPAN)

    def slice_at(owner):
        return pl.ds(pl.multiple_of(owner * rows, rows), rows)

    def load_w(i):
        owner = lax.rem(place + i, shards)
        return pltpu.make_async_copy(
            w_hbm.at[slice_at(owner), :], w_ref.at[me, slice_at(owner), :], w_sem.at[i]
        )

    def load_x(c):
        return pltpu.make_async_copy(x_hbm.at[span_at(c), :], x_ref.at[span_at(c), :], x_sem.at[c])

    def load_g(c):
        return pltpu.make_async_copy(g_hbm.at[span_at(c), :], g_ref.at[span_at(c), :], g_sem.at[c])

    smalls = [
        pltpu.make_async_copy(src, dst, in_sem.at[i])
        for i, (src, dst) in enumerate(
            ((st_hbm, st_ref), (dr_hbm, dr_ref), (b_hbm, b_ref), (c_hbm, c_ref))
        )
    ]

    moves = weight_moves(ranks)

    def along(owner, dest, part):
        low = rows // 32 * 16
        at = pl.ds(
            pl.multiple_of(place * rows + (low if part else 0), 8), rows - low if part else low
        )
        return pltpu.make_async_remote_copy(
            src_ref=w_ref.at[owner, at, :],
            dst_ref=w_ref.at[owner, at, :],
            send_sem=along_s.at[owner, dest, part],
            recv_sem=along_r.at[owner, part],
            device_id={"head": dest},
            device_id_type=MESH,
        )

    def move(now):
        for h in range(ranks):
            mine = [(r, b, part) for r, a, b, part, phase in moves if a == h and phase == now]
            if mine:

                @pl.when(me == h)
                def _(h=h, mine=mine):
                    for r, b, part in mine:
                        if r != h:
                            along(r, b, part).wait_recv()
                        along(r, b, part).start()

    def spread_out(early):
        for h in range(ranks):
            relayed = [r for r, a, b, part, phase in moves if a == h and r != h]
            outer = ranks == 4 and h in (0, ranks - 1)
            owners = near_order(ranks)[h]
            if outer:
                owners = owners[:1] if early else owners[1:]
            elif not early:
                owners = []
            if owners:

                @pl.when(me == h)
                def _(h=h, relayed=relayed, owners=owners):
                    for r in owners:
                        if r not in relayed:
                            for part in (0, 1):
                                along(r, r, part).wait_recv()
                        spread_plane(jnp.int32(r))

    square = chips == 4
    direct = (1, 2) if square else tuple(range(1, chips))

    def chip_to(j):
        if square:
            return (chip, chip + 1 - 2 * lax.rem(chip, 2), lax.rem(chip + 2, 4), 3 - chip)[j]
        return lax.rem(chip + j, chips)

    def chip_from(j):
        return chip_to(j) if square else lax.rem(chip - j + chips, chips)

    def over_chips(low, one):
        if square:
            for j in range(low, chips):
                one(j)
        else:

            def step(j, carry):
                one(j)
                return carry

            lax.fori_loop(low, chips, step, 0)

    def plane(r, j):
        slot = lax.rem(r - me + ranks, ranks) - 1
        dest = chip_to(j) * 2 + core
        return pltpu.make_async_remote_copy(
            src_ref=w_ref.at[r, slice_at(place), :],
            dst_ref=w_ref.at[r, slice_at(place), :],
            send_sem=plane_s.at[slot, j],
            recv_sem=plane_r.at[slot, j],
            device_id={"seq": dest},
            device_id_type=MESH,
        )

    def landed(r, j):
        slot = lax.rem(r - me + ranks, ranks) - 1
        owner = chip_from(j) * 2 + core
        return pltpu.make_async_remote_copy(
            src_ref=w_ref.at[r, slice_at(owner), :],
            dst_ref=w_ref.at[r, slice_at(owner), :],
            send_sem=plane_s.at[slot, j],
            recv_sem=plane_r.at[slot, j],
            device_id={"seq": owner},
            device_id_type=MESH,
        )

    def corner(r, part, dest, owner):
        slot = lax.rem(r - me + ranks, ranks) - 1
        low = rows // 32 * 16
        at = pl.ds(
            pl.multiple_of((owner * 2 + core) * rows + (low if part else 0), 16),
            rows - low if part else low,
        )
        return pltpu.make_async_remote_copy(
            src_ref=w_ref.at[r, at, :],
            dst_ref=w_ref.at[r, at, :],
            send_sem=plane_s.at[slot, 3 * part],
            recv_sem=plane_r.at[slot, 3 * part],
            device_id={"seq": dest * 2 + core},
            device_id_type=MESH,
        )

    def turn(r, part):
        return corner(r, part, chip_to(2 - part), chip_to(1 + part))

    def turned(r, part):
        return corner(r, part, chip_to(2 - part), chip_to(3))

    def across(r, j, of_core):
        slot = lax.rem(r - me + ranks, ranks) - 1
        owner = chip_from(j) * 2 + of_core
        return pltpu.make_async_remote_copy(
            src_ref=w_ref.at[r, slice_at(owner), :],
            dst_ref=w_ref.at[r, slice_at(owner), :],
            send_sem=sib_s.at[slot, j],
            recv_sem=sib_r.at[slot, j],
            device_id={"seq": sibling},
            device_id_type=MESH,
        )

    def spread_plane(r):
        across(r, 0, core).start()
        if square:
            for j in direct:
                plane(r, j).start()
        else:
            over_chips(1, lambda j: plane(r, j).start())

    load_w(0).start()
    for copy in smalls[:3]:
        copy.start()

    def load_xs(c, carry):
        load_x(c).start()
        return carry

    lax.fori_loop(0, blocks, load_xs, 0)
    smalls[3].start()

    barrier = pltpu.get_barrier_semaphore()

    def greet(k, carry):
        pl.semaphore_signal(
            barrier, inc=1, device_id={"head": lax.rem(me + k, ranks)}, device_id_type=MESH
        )
        return carry

    def greet_plane(j):
        dest = chip_to(j) * 2 + core
        pl.semaphore_signal(barrier, inc=1, device_id={"seq": dest}, device_id_type=MESH)

    lax.fori_loop(1, ranks, greet, 0)
    over_chips(1, greet_plane)
    pl.semaphore_signal(barrier, inc=1, device_id={"seq": sibling}, device_id_type=MESH)
    pl.semaphore_wait(barrier, ranks - 1 + chips)

    load_w(0).wait()

    move(0)

    i0 = lax.broadcasted_iota(jnp.int32, (SPAN, SPAN), 0)
    i1 = lax.broadcasted_iota(jnp.int32, (SPAN, SPAN), 1)
    lower = i0 >= i1
    tril = jnp.where(lower, 1.0, 0.0).astype(F32)
    spread = expander(heads, width)
    spread16 = spread.astype(BF16)
    s_ref[...] = jnp.zeros_like(s_ref)
    l_ref[...] = jnp.ones_like(l_ref)
    for copy in smalls[:3]:
        copy.wait()

    def scan(c, carry):
        at = span_at(c)
        load_x(c).wait()
        load_g(c).start()
        slot = c * SPAN + lax.broadcasted_iota(jnp.int32, (heads, SPAN), 1)
        live = slot < valid
        ld = jnp.where(live, dr_ref[:, at] * (-LOG2E), 0.0)
        run = contract(ld, tril, 1, 1, HIGH)
        runT = contract(tril, ld, 1, 1, HIGH)
        q = jnp.where(live, run - jnp.log2(st_ref[:, at]), 1e30)
        runT_ref[at, :] = runT
        q_ref[:, at] = q
        tail = jnp.exp2(run[:, SPAN - 1 :] - q)
        hi, lo = halves(tail)
        texp = contract(hi, spread16, 0, 0) + contract(lo, spread16, 0, 0)
        weighted = (x_ref[at, :].astype(F32) * texp).astype(BF16)
        fresh = contract(b_ref[at, :], weighted, 0, 0)
        dec = contract(jnp.exp2(runT[SPAN - 8 :, :]), spread, 1, 0, HIGH)[7:8, :]
        before_ref[c] = s_ref[...]
        lead_ref[c] = l_ref[...]
        s_ref[...] = dec * s_ref[...] + fresh
        l_ref[...] = l_ref[...] * dec
        return carry

    lax.fori_loop(0, blocks, scan, 0)
    move(1)
    mine_ref[0:state, :] = s_ref[...].astype(BF16)
    mine_ref[state:, :] = pack_rows(l_ref[0:1, :])

    pair = pltpu.make_async_remote_copy(
        src_ref=mine_ref,
        dst_ref=other_ref,
        send_sem=pair_s.at[0],
        recv_sem=pair_r.at[0],
        device_id={"seq": sibling},
        device_id_type=MESH,
    )
    pair.start()

    def load_ws(i, carry):
        load_w(i).start()
        return carry

    lax.fori_loop(1, shards, load_ws, 0)
    pair.wait()
    cols = pl.ds(pl.multiple_of(core * half, half), half)
    own = mine_ref[:, cols].astype(F32)
    peer = other_ref[:, cols].astype(F32)
    first = jnp.where(core == 0, own, peer)
    second = jnp.where(core == 0, peer, own)
    first_dec = unpack_rows(first[state:, :])
    second_dec = unpack_rows(second[state:, :])
    chip_ref[0:state, :] = (second_dec * first[0:state, :] + second[0:state, :]).astype(BF16)
    chip_ref[state:, :] = pack_rows(first_dec * second_dec)

    def to_chip(j, other):
        return pltpu.make_async_remote_copy(
            src_ref=chip_ref,
            dst_ref=chips_ref.at[j],
            send_sem=chip_s.at[j],
            recv_sem=chip_r.at[j],
            device_id={"seq": other * 2 + core},
            device_id_type=MESH,
        )

    def tell(j, carry):
        @pl.when(chip + j < chips)
        def _():
            to_chip(j, chip + j).start()

        return carry

    lax.fori_loop(1, chips, tell, 0)
    move(2)
    inc_ref[:, cols] = jnp.zeros((state, half), F32)

    def hear(i, carry):
        j = chips - i

        @pl.when(j <= chip)
        def _():
            to_chip(j, chip - j).wait_recv()
            block = chips_ref[j]
            decay = unpack_rows(block[state:, :])
            inc_ref[:, cols] = decay * inc_ref[:, cols] + block[0:state, :].astype(F32)

        return carry

    lax.fori_loop(1, chips, hear, 0)
    swap = pltpu.make_async_remote_copy(
        src_ref=inc_ref.at[:, cols],
        dst_ref=inc_ref.at[:, cols],
        send_sem=pair_s.at[1],
        recv_sem=pair_r.at[1],
        device_id={"seq": sibling},
        device_id_type=MESH,
    )
    swap.start()
    swap.wait()
    inc = inc_ref[...]
    after = unpack_rows(other_ref[state:, :]) * inc + other_ref[0:state, :].astype(F32)
    inc_ref[...] = jnp.where(core == 1, after, inc)

    smalls[3].wait()
    left = lax.broadcasted_iota(jnp.int32, (SPAN, 128), 1) < (width // heads)
    ones = jnp.ones((8, 128), F32)

    def copies(dest, j, slot):
        c = dest * each + j
        big = pltpu.make_async_remote_copy(
            src_ref=g_ref.at[span_at(c), :],
            dst_ref=got_ref.at[slot, pl.ds(j * SPAN, SPAN), :],
            send_sem=send_sem.at[slot, j],
            recv_sem=recv_sem.at[slot, j],
            device_id={"head": dest},
            device_id_type=MESH,
        )
        small = pltpu.make_async_remote_copy(
            src_ref=ss_buf.at[c],
            dst_ref=ss_ref.at[slot, j],
            send_sem=ssend_sem.at[slot, j],
            recv_sem=srecv_sem.at[slot, j],
            device_id={"head": dest},
            device_id_type=MESH,
        )
        return big, small

    def span(c):
        at = span_at(c)
        load_g(c).wait()
        cb = c_ref[at, :]
        gram = jnp.where(lower, contract(cb, b_ref[at, :], 1, 1), 0.0)
        held = (before_ref[c] + lead_ref[c, 0:1, :] * inc_ref[...]).astype(BF16)
        runT = runT_ref[at, :]
        q = q_ref[:, at]
        hi, lo = halves(jnp.exp2(runT))
        acc = jnp.zeros((SPAN, 128), F32)
        for p in range(width // 128):
            lanes = slice(p * 128, p * 128 + 128)
            xp = x_ref[at, lanes]
            grow = contract(hi, spread16[:, lanes], 1, 0) + contract(lo, spread16[:, lanes], 1, 0)
            carried = contract(cb, held[:, lanes], 1, 0) * grow
            sides = []
            for h in (2 * p, 2 * p + 1):
                m = (
                    gram * jnp.exp2(jnp.minimum(runT[:, h : h + 1] - q[h : h + 1, :], 0.0))
                ).astype(BF16)
                sides.append(jnp.dot(m, xp, preferred_element_type=F32))
            inner = jnp.where(left, sides[0], sides[1])
            z = g_ref[at, lanes].astype(F32)
            skip = jnp.where(left[0:1, :], skip_ref[2 * p], skip_ref[2 * p + 1])
            gated = (inner + carried + skip * xp.astype(F32)) * (
                z * (0.5 * jnp.tanh(0.5 * z) + 0.5)
            )
            acc = acc + gated * gated
            g_ref[at, lanes] = (gated * gain_ref[lanes][None, :]).astype(BF16)
        ss_buf[c] = contract(ones, acc, 1, 1, HIGH)

    if ranks == 4:
        order = [ranks - 1 - me, lax.rem(me + 2, ranks), me + 1 - 2 * lax.rem(me, 2)]
    else:
        order = [lax.rem(me + k, ranks) for k in range(1, ranks)]
    for index, dest in enumerate(order):
        slot = lax.rem(me - dest + ranks, ranks) - 1

        def one(j, carry, dest=dest, slot=slot):
            span(dest * each + j)
            for copy in copies(dest, j, slot):
                copy.start()
            return carry

        lax.fori_loop(0, each, one, 0)
        if index == 0:
            move(3)
            spread_out(True)

    def mine(j, carry):
        span(me * each + j)
        return carry

    lax.fori_loop(0, each, mine, 0)

    def wait_ws(i, carry):
        load_w(i).wait()
        return carry

    lax.fori_loop(1, shards, wait_ws, 0)
    local = pl.ds(pl.multiple_of(me * share, share), share)

    def own_tile(n, carry):
        lanes = pl.ds(pl.multiple_of(n * TILE, TILE), TILE)
        acc_ref[:, lanes] = jnp.dot(
            g_ref[local, :], w_ref[me, :, lanes], preferred_element_type=F32
        )
        return carry

    lax.fori_loop(0, tiles, own_tile, 0)

    near = near_order(ranks)
    late = late_order(ranks)

    def source_of(table, i):
        return pick([row[i] for row in table], me)

    def pass_direct(i):
        r = source_of(near, i)
        if square:
            for j in direct:
                landed(r, j).wait_recv()
                turn(r, j - 1).start()
                across(r, j, core).start()
        else:

            def one(j):
                landed(r, j).wait_recv()
                across(r, j, core).start()

            over_chips(1, one)

    def pass_corner(i):
        r = source_of(near, i)
        if square:
            for part in (0, 1):
                turned(r, part).wait_recv()
            across(r, 3, core).start()
        over_chips(0, lambda j: across(r, j, 1 - core).wait_recv())

    pass_direct(0)
    spread_out(False)
    for i in range(1, ranks - 1):
        pass_direct(i)
        pass_corner(i - 1)
    pass_corner(ranks - 2)

    def take(i):
        r = source_of(late, i)
        return r, lax.rem(r - me + ranks, ranks) - 1

    def receive(r, slot, j):
        for copy in copies(r, j, slot):
            copy.wait_recv()

    for i in range(ranks - 2):
        r, slot = take(i)
        for j in range(each):
            receive(r, slot, j)

        def more(n, carry, r=r, slot=slot):
            lanes = pl.ds(pl.multiple_of(n * TILE, TILE), TILE)
            acc_ref[:, lanes] += jnp.dot(
                got_ref[slot], w_ref[r, :, lanes], preferred_element_type=F32
            )
            return carry

        lax.fori_loop(0, tiles, more, 0)

    r, slot = take(ranks - 2)
    unit = jnp.where(lax.broadcasted_iota(jnp.int32, (8, 128), 0) == 0, 1.0, 0.0).astype(F32)

    def put(n, j):
        lanes = pl.ds(pl.multiple_of(n * TILE, TILE), TILE)
        at = pl.ds(j * SPAN, SPAN)
        return pltpu.make_async_copy(
            res_ref.at[at, lanes], out_hbm.at[at, lanes], out_sem.at[n, j]
        )

    for j in range(each):
        receive(r, slot, j)
        total = ss_buf[me * each + j]
        for k in range(ranks - 1):
            total = total + ss_ref[k, j]
        column = contract(total, unit, 0, 0, HIGH) * (1.0 / (width * ranks))
        token = me * share + j * SPAN + lax.broadcasted_iota(jnp.int32, (SPAN, 128), 0)
        scale = jnp.where(token < valid, lax.rsqrt(column + 1e-05), 0.0)
        wide = jnp.concatenate([scale] * (TILE // 128), axis=1)
        at = pl.ds(j * SPAN, SPAN)

        def final(n, carry, j=j, at=at, wide=wide):
            lanes = pl.ds(pl.multiple_of(n * TILE, TILE), TILE)
            part = jnp.dot(got_ref[slot, at, :], w_ref[r, :, lanes], preferred_element_type=F32)
            res_ref[at, lanes] = ((acc_ref[at, lanes] + part) * wide).astype(BF16)
            put(n, j).start()
            return carry

        lax.fori_loop(0, tiles, final, 0)

    for h in range(ranks):

        @pl.when(me == h)
        def _(h=h):
            for r, a, b, part, phase in moves:
                if a == h:
                    along(r, b, part).wait_send()

    for i in range(ranks - 1):
        r = source_of(near, i)
        if square:
            for j in direct:
                plane(r, j).wait_send()
                turn(r, j - 1).wait_send()
        else:
            over_chips(1, lambda j: plane(r, j).wait_send())
        over_chips(0, lambda j: across(r, j, core).wait_send())

    def told(j, carry):
        @pl.when(chip + j < chips)
        def _():
            to_chip(j, chip + j).wait_send()

        return carry

    lax.fori_loop(1, chips, told, 0)
    for dest in order:
        slot = lax.rem(me - dest + ranks, ranks) - 1

        def sent(j, carry, dest=dest, slot=slot):
            for copy in copies(dest, j, slot):
                copy.wait_send()
            return carry

        lax.fori_loop(0, each, sent, 0)

    def wait_put(n, carry):
        for j in range(each):
            put(n, j).wait()
        return carry

    lax.fori_loop(0, tiles, wait_put, 0)


def body(
    ranks,
    shards,
    values,
    gates,
    b_proj,
    c_proj,
    step_size,
    decay_rate,
    skip_gain,
    norm_gain,
    readout,
    span_counts,
    remaining_count,
):
    length, width = values.shape
    heads = step_size.shape[0]
    state = b_proj.shape[1]
    depth = readout.shape[1]
    blocks = length // SPAN
    share = length // ranks
    each = blocks // ranks
    chips = shards // 2
    sds = jax.ShapeDtypeStruct
    smem = pl.BlockSpec(memory_space=pltpu.SMEM)
    hbm = pl.BlockSpec(memory_space=pl.ANY)
    dma = pltpu.SemaphoreType.DMA
    return pl.pallas_call(
        functools.partial(layer_kernel, ranks, shards),
        out_shape=sds((share, depth), BF16),
        in_specs=[smem, smem, smem, pl.BlockSpec(memory_space=VMEM)] + [hbm] * 7,
        out_specs=hbm,
        scratch_shapes=[
            VMEM((length, width), BF16),
            VMEM((length, width), BF16),
            VMEM((length, state), BF16),
            VMEM((length, state), BF16),
            VMEM((heads, length), F32),
            VMEM((heads, length), F32),
            VMEM((length, heads), F32),
            VMEM((heads, length), F32),
            VMEM((blocks, state, width), F32),
            VMEM((blocks, 8, width), F32),
            VMEM((state, width), F32),
            VMEM((8, width), F32),
            VMEM((state + 16, width), BF16),
            VMEM((state + 16, width), BF16),
            VMEM((state + 16, width // 2), BF16),
            VMEM((chips, state + 16, width // 2), BF16),
            VMEM((state, width), F32),
            VMEM((ranks, width, depth), BF16),
            VMEM((ranks - 1, share, width), BF16),
            VMEM((blocks, 8, SPAN), F32),
            VMEM((ranks - 1, each, 8, SPAN), F32),
            VMEM((share, depth), F32),
            VMEM((share, depth), BF16),
            dma((blocks,)),
            dma((blocks,)),
            dma((4,)),
            dma((shards,)),
            dma((ranks, ranks, 2)),
            dma((ranks, 2)),
            dma((ranks - 1, chips)),
            dma((ranks - 1, chips)),
            dma((ranks - 1, chips)),
            dma((ranks - 1, chips)),
            dma((2,)),
            dma((2,)),
            dma((chips,)),
            dma((chips,)),
            dma((ranks - 1, each)),
            dma((ranks - 1, each)),
            dma((ranks - 1, each)),
            dma((ranks - 1, each)),
            dma((depth // TILE, each)),
        ],
        compiler_params=pltpu.CompilerParams(
            vmem_limit_bytes=LIMIT, collective_id=0, has_side_effects=True
        ),
        cost_estimate=pl.CostEstimate(
            flops=10**11, bytes_accessed=20 * 10**6, transcendentals=0
        ),
        name="layer",
    )(
        span_counts,
        remaining_count,
        skip_gain,
        norm_gain,
        values,
        gates,
        b_proj,
        c_proj,
        step_size,
        decay_rate,
        readout,
    )


def solution(mesh):
    return jax.shard_map(
        functools.partial(body, mesh.shape["head"], mesh.shape["seq"]),
        mesh=mesh,
        in_specs=(
            P("seq", "head"),
            P("seq", "head"),
            P("seq", None),
            P("seq", None),
            P("head", "seq"),
            P("head", "seq"),
            P("head"),
            P("head"),
            P("head", None),
            P("seq"),
            P("seq"),
        ),
        out_specs=P(("seq", "head"), None),
        check_vma=False,
    )
```

```python
import functools
import math

import jax
import jax.numpy as jnp
from jax import lax
from jax.experimental import pallas as pl
from jax.experimental.pallas import tpu as pltpu
from jax.sharding import PartitionSpec as P

SPAN = 256
LOG2E = math.log2(math.e)
F32 = jnp.float32
BF16 = jnp.bfloat16
HIGH = lax.Precision.HIGHEST
MESH = pl.DeviceIdType.MESH
VMEM = pltpu.VMEM
LIMIT = 63 * 1024 * 1024
TILE = 512


def contract(a, b, da, db, precision=None):
    return lax.dot_general(
        a, b, (((da,), (db,)), ((), ())), precision=precision, preferred_element_type=F32
    )


def expander(heads, width):
    size = width // heads
    col = lax.broadcasted_iota(jnp.int32, (heads, width), 1) // size
    row = lax.broadcasted_iota(jnp.int32, (heads, width), 0)
    return jnp.where(col == row, 1.0, 0.0).astype(F32)


def halves(a):
    hi = a.astype(BF16)
    return hi, (a - hi.astype(F32)).astype(BF16)


def pack_rows(total):
    total = jnp.broadcast_to(total, (16, total.shape[1]))
    hi, mid = halves(total)
    low = (total - hi.astype(F32) - mid.astype(F32)).astype(BF16)
    row = lax.broadcasted_iota(jnp.int32, total.shape, 0)
    parts = jnp.where(row == 0, hi.astype(F32), jnp.where(row == 1, mid.astype(F32), low.astype(F32)))
    return jnp.where(row < 3, parts, 0.0).astype(BF16)


def unpack_rows(rows):
    rows = rows.astype(F32)
    return rows[0:1, :] + rows[1:2, :] + rows[2:3, :]


def pick(table, index):
    total = jnp.int32(0)
    for i, value in enumerate(table):
        total = total + jnp.where(index == i, jnp.int32(value), jnp.int32(0))
    return total


def near_order(ranks):
    return [sorted((r for r in range(ranks) if r != h), key=lambda r: (abs(r - h), r)) for h in range(ranks)]


def weight_moves(ranks):
    if ranks != 4:
        return [
            (r, r, t, part, 0) for part in (0, 1) for r in range(ranks) for t in range(ranks) if t != r
        ]
    right = [(0, 0, 2, 0, 0), (0, 0, 2, 1, 0), (0, 0, 1, 0, 0), (0, 0, 1, 1, 0)]
    right += [(2, 2, 3, 0, 0), (2, 2, 3, 1, 0), (1, 1, 2, 0, 0), (1, 1, 2, 1, 0)]
    right += [(0, 2, 3, 0, 1), (0, 2, 3, 1, 2), (1, 2, 3, 0, 3), (1, 2, 3, 1, 3)]
    return right + [(3 - r, 3 - a, 3 - b, part, phase) for r, a, b, part, phase in right]


def late_order(ranks):
    if ranks == 4:
        return [[1, 3, 2], [0, 3, 2], [3, 0, 1], [2, 0, 1]]
    return near_order(ranks)


def layer_kernel(
    ranks,
    shards,
    count_ref,
    remain_ref,
    skip_ref,
    gain_ref,
    x_hbm,
    g_hbm,
    b_hbm,
    c_hbm,
    st_hbm,
    dr_hbm,
    w_hbm,
    out_hbm,
    x_ref,
    g_ref,
    b_ref,
    c_ref,
    st_ref,
    dr_ref,
    runT_ref,
    q_ref,
    before_ref,
    lead_ref,
    s_ref,
    l_ref,
    mine_ref,
    other_ref,
    chip_ref,
    chips_ref,
    inc_ref,
    w_ref,
    got_ref,
    ss_buf,
    ss_ref,
    acc_ref,
    res_ref,
    x_sem,
    g_sem,
    in_sem,
    w_sem,
    along_s,
    along_r,
    plane_s,
    plane_r,
    sib_s,
    sib_r,
    pair_s,
    pair_r,
    chip_s,
    chip_r,
    send_sem,
    recv_sem,
    ssend_sem,
    srecv_sem,
    out_sem,
):
    heads, length = q_ref.shape
    width = x_ref.shape[1]
    blocks = length // SPAN
    each = blocks // ranks
    share = length // ranks
    state = s_ref.shape[0]
    depth = res_ref.shape[1]
    rows = width // shards
    chips = shards // 2
    half = width // 2
    tiles = depth // TILE
    me = lax.axis_index("head")
    place = lax.axis_index("seq")
    core = lax.rem(place, 2)
    chip = lax.div(place, 2)
    sibling = place + 1 - 2 * core
    valid = (count_ref[0] - 1) * SPAN + remain_ref[0]

    def span_at(c):
        return pl.ds(pl.multiple_of(c * SPAN, SPAN), SPAN)

    def slice_at(owner):
        return pl.ds(pl.multiple_of(owner * rows, rows), rows)

    def load_w(i):
        owner = lax.rem(place + i, shards)
        return pltpu.make_async_copy(
            w_hbm.at[slice_at(owner), :], w_ref.at[me, slice_at(owner), :], w_sem.at[i]
        )

    def load_x(c):
        return pltpu.make_async_copy(x_hbm.at[span_at(c), :], x_ref.at[span_at(c), :], x_sem.at[c])

    def load_g(c):
        return pltpu.make_async_copy(g_hbm.at[span_at(c), :], g_ref.at[span_at(c), :], g_sem.at[c])

    smalls = [
        pltpu.make_async_copy(src, dst, in_sem.at[i])
        for i, (src, dst) in enumerate(
            ((st_hbm, st_ref), (dr_hbm, dr_ref), (b_hbm, b_ref), (c_hbm, c_ref))
        )
    ]

    moves = weight_moves(ranks)

    def along(owner, dest, part):
        low = rows // 32 * 16
        at = pl.ds(
            pl.multiple_of(place * rows + (low if part else 0), 8), rows - low if part else low
        )
        return pltpu.make_async_remote_copy(
            src_ref=w_ref.at[owner, at, :],
            dst_ref=w_ref.at[owner, at, :],
            send_sem=along_s.at[owner, dest, part],
            recv_sem=along_r.at[owner, part],
            device_id={"head": dest},
            device_id_type=MESH,
        )

    def move(now):
        for h in range(ranks):
            mine = [(r, b, part) for r, a, b, part, phase in moves if a == h and phase == now]
            if mine:

                @pl.when(me == h)
                def _(h=h, mine=mine):
                    for r, b, part in mine:
                        if r != h:
                            along(r, b, part).wait_recv()
                        along(r, b, part).start()

    def spread_out(early):
        for h in range(ranks):
            relayed = [r for r, a, b, part, phase in moves if a == h and r != h]
            outer = ranks == 4 and h in (0, ranks - 1)
            owners = near_order(ranks)[h]
            if outer:
                owners = owners[:1] if early else owners[1:]
            elif not early:
                owners = []
            if owners:

                @pl.when(me == h)
                def _(h=h, relayed=relayed, owners=owners):
                    for r in owners:
                        if r not in relayed:
                            for part in (0, 1):
                                along(r, r, part).wait_recv()
                        spread_plane(jnp.int32(r))

    square = chips == 4
    direct = (1, 2) if square else tuple(range(1, chips))

    def chip_to(j):
        if square:
            return (chip, chip + 1 - 2 * lax.rem(chip, 2), lax.rem(chip + 2, 4), 3 - chip)[j]
        return lax.rem(chip + j, chips)

    def chip_from(j):
        return chip_to(j) if square else lax.rem(chip - j + chips, chips)

    def over_chips(low, one):
        if square:
            for j in range(low, chips):
                one(j)
        else:

            def step(j, carry):
                one(j)
                return carry

            lax.fori_loop(low, chips, step, 0)

    def plane(r, j):
        slot = lax.rem(r - me + ranks, ranks) - 1
        dest = chip_to(j) * 2 + core
        return pltpu.make_async_remote_copy(
            src_ref=w_ref.at[r, slice_at(place), :],
            dst_ref=w_ref.at[r, slice_at(place), :],
            send_sem=plane_s.at[slot, j],
            recv_sem=plane_r.at[slot, j],
            device_id={"seq": dest},
            device_id_type=MESH,
        )

    def landed(r, j):
        slot = lax.rem(r - me + ranks, ranks) - 1
        owner = chip_from(j) * 2 + core
        return pltpu.make_async_remote_copy(
            src_ref=w_ref.at[r, slice_at(owner), :],
            dst_ref=w_ref.at[r, slice_at(owner), :],
            send_sem=plane_s.at[slot, j],
            recv_sem=plane_r.at[slot, j],
            device_id={"seq": owner},
            device_id_type=MESH,
        )

    def corner(r, part, dest, owner):
        slot = lax.rem(r - me + ranks, ranks) - 1
        low = rows // 32 * 16
        at = pl.ds(
            pl.multiple_of((owner * 2 + core) * rows + (low if part else 0), 16),
            rows - low if part else low,
        )
        return pltpu.make_async_remote_copy(
            src_ref=w_ref.at[r, at, :],
            dst_ref=w_ref.at[r, at, :],
            send_sem=plane_s.at[slot, 3 * part],
            recv_sem=plane_r.at[slot, 3 * part],
            device_id={"seq": dest * 2 + core},
            device_id_type=MESH,
        )

    def turn(r, part):
        return corner(r, part, chip_to(2 - part), chip_to(1 + part))

    def turned(r, part):
        return corner(r, part, chip_to(2 - part), chip_to(3))

    def across(r, j, of_core):
        slot = lax.rem(r - me + ranks, ranks) - 1
        owner = chip_from(j) * 2 + of_core
        return pltpu.make_async_remote_copy(
            src_ref=w_ref.at[r, slice_at(owner), :],
            dst_ref=w_ref.at[r, slice_at(owner), :],
            send_sem=sib_s.at[slot, j],
            recv_sem=sib_r.at[slot, j],
            device_id={"seq": sibling},
            device_id_type=MESH,
        )

    def spread_plane(r):
        across(r, 0, core).start()
        if square:
            for j in direct:
                plane(r, j).start()
        else:
            over_chips(1, lambda j: plane(r, j).start())

    load_w(0).start()
    for copy in smalls[:3]:
        copy.start()

    def load_xs(c, carry):
        load_x(c).start()
        return carry

    lax.fori_loop(0, blocks, load_xs, 0)
    smalls[3].start()

    barrier = pltpu.get_barrier_semaphore()

    def greet(k, carry):
        pl.semaphore_signal(
            barrier, inc=1, device_id={"head": lax.rem(me + k, ranks)}, device_id_type=MESH
        )
        return carry

    def greet_plane(j):
        dest = chip_to(j) * 2 + core
        pl.semaphore_signal(barrier, inc=1, device_id={"seq": dest}, device_id_type=MESH)

    lax.fori_loop(1, ranks, greet, 0)
    over_chips(1, greet_plane)
    pl.semaphore_signal(barrier, inc=1, device_id={"seq": sibling}, device_id_type=MESH)
    pl.semaphore_wait(barrier, ranks - 1 + chips)

    load_w(0).wait()

    move(0)

    i0 = lax.broadcasted_iota(jnp.int32, (SPAN, SPAN), 0)
    i1 = lax.broadcasted_iota(jnp.int32, (SPAN, SPAN), 1)
    lower = i0 >= i1
    tril = jnp.where(lower, 1.0, 0.0).astype(F32)
    spread = expander(heads, width)
    spread16 = spread.astype(BF16)
    s_ref[...] = jnp.zeros_like(s_ref)
    l_ref[...] = jnp.ones_like(l_ref)
    for copy in smalls[:3]:
        copy.wait()

    def scan(c, carry):
        at = span_at(c)
        load_x(c).wait()
        load_g(c).start()
        slot = c * SPAN + lax.broadcasted_iota(jnp.int32, (heads, SPAN), 1)
        live = slot < valid
        ld = jnp.where(live, dr_ref[:, at] * (-LOG2E), 0.0)
        run = contract(ld, tril, 1, 1, HIGH)
        runT = contract(tril, ld, 1, 1, HIGH)
        q = jnp.where(live, run - jnp.log2(st_ref[:, at]), 1e30)
        runT_ref[at, :] = runT
        q_ref[:, at] = q
        tail = jnp.exp2(run[:, SPAN - 1 :] - q)
        hi, lo = halves(tail)
        texp = contract(hi, spread16, 0, 0) + contract(lo, spread16, 0, 0)
        weighted = (x_ref[at, :].astype(F32) * texp).astype(BF16)
        fresh = contract(b_ref[at, :], weighted, 0, 0)
        dec = contract(jnp.exp2(runT[SPAN - 8 :, :]), spread, 1, 0, HIGH)[7:8, :]
        before_ref[c] = s_ref[...]
        lead_ref[c] = l_ref[...]
        s_ref[...] = dec * s_ref[...] + fresh
        l_ref[...] = l_ref[...] * dec
        return carry

    lax.fori_loop(0, blocks, scan, 0)
    move(1)
    mine_ref[0:state, :] = s_ref[...].astype(BF16)
    mine_ref[state:, :] = pack_rows(l_ref[0:1, :])

    pair = pltpu.make_async_remote_copy(
        src_ref=mine_ref,
        dst_ref=other_ref,
        send_sem=pair_s.at[0],
        recv_sem=pair_r.at[0],
        device_id={"seq": sibling},
        device_id_type=MESH,
    )
    pair.start()

    def load_ws(i, carry):
        load_w(i).start()
        return carry

    lax.fori_loop(1, shards, load_ws, 0)
    pair.wait()
    cols = pl.ds(pl.multiple_of(core * half, half), half)
    own = mine_ref[:, cols].astype(F32)
    peer = other_ref[:, cols].astype(F32)
    first = jnp.where(core == 0, own, peer)
    second = jnp.where(core == 0, peer, own)
    first_dec = unpack_rows(first[state:, :])
    second_dec = unpack_rows(second[state:, :])
    chip_ref[0:state, :] = (second_dec * first[0:state, :] + second[0:state, :]).astype(BF16)
    chip_ref[state:, :] = pack_rows(first_dec * second_dec)

    def to_chip(j, other):
        return pltpu.make_async_remote_copy(
            src_ref=chip_ref,
            dst_ref=chips_ref.at[j],
            send_sem=chip_s.at[j],
            recv_sem=chip_r.at[j],
            device_id={"seq": other * 2 + core},
            device_id_type=MESH,
        )

    def tell(j, carry):
        @pl.when(chip + j < chips)
        def _():
            to_chip(j, chip + j).start()

        return carry

    lax.fori_loop(1, chips, tell, 0)
    move(2)
    inc_ref[:, cols] = jnp.zeros((state, half), F32)

    def hear(i, carry):
        j = chips - i

        @pl.when(j <= chip)
        def _():
            to_chip(j, chip - j).wait_recv()
            block = chips_ref[j]
            decay = unpack_rows(block[state:, :])
            inc_ref[:, cols] = decay * inc_ref[:, cols] + block[0:state, :].astype(F32)

        return carry

    lax.fori_loop(1, chips, hear, 0)
    swap = pltpu.make_async_remote_copy(
        src_ref=inc_ref.at[:, cols],
        dst_ref=inc_ref.at[:, cols],
        send_sem=pair_s.at[1],
        recv_sem=pair_r.at[1],
        device_id={"seq": sibling},
        device_id_type=MESH,
    )
    swap.start()
    swap.wait()
    inc = inc_ref[...]
    after = unpack_rows(other_ref[state:, :]) * inc + other_ref[0:state, :].astype(F32)
    inc_ref[...] = jnp.where(core == 1, after, inc)

    smalls[3].wait()
    left = lax.broadcasted_iota(jnp.int32, (SPAN, 128), 1) < (width // heads)
    ones = jnp.ones((8, 128), F32)

    def copies(dest, j, slot):
        c = dest * each + j
        big = pltpu.make_async_remote_copy(
            src_ref=g_ref.at[span_at(c), :],
            dst_ref=got_ref.at[slot, pl.ds(j * SPAN, SPAN), :],
            send_sem=send_sem.at[slot, j],
            recv_sem=recv_sem.at[slot, j],
            device_id={"head": dest},
            device_id_type=MESH,
        )
        small = pltpu.make_async_remote_copy(
            src_ref=ss_buf.at[c],
            dst_ref=ss_ref.at[slot, j],
            send_sem=ssend_sem.at[slot, j],
            recv_sem=srecv_sem.at[slot, j],
            device_id={"head": dest},
            device_id_type=MESH,
        )
        return big, small

    def span(c):
        at = span_at(c)
        load_g(c).wait()
        cb = c_ref[at, :]
        gram = jnp.where(lower, contract(cb, b_ref[at, :], 1, 1), 0.0)
        held = (before_ref[c] + lead_ref[c, 0:1, :] * inc_ref[...]).astype(BF16)
        runT = runT_ref[at, :]
        q = q_ref[:, at]
        hi, lo = halves(jnp.exp2(runT))
        acc = jnp.zeros((SPAN, 128), F32)
        for p in range(width // 128):
            lanes = slice(p * 128, p * 128 + 128)
            xp = x_ref[at, lanes]
            grow = contract(hi, spread16[:, lanes], 1, 0) + contract(lo, spread16[:, lanes], 1, 0)
            carried = contract(cb, held[:, lanes], 1, 0) * grow
            sides = []
            for h in (2 * p, 2 * p + 1):
                m = (
                    gram * jnp.exp2(jnp.minimum(runT[:, h : h + 1] - q[h : h + 1, :], 0.0))
                ).astype(BF16)
                sides.append(jnp.dot(m, xp, preferred_element_type=F32))
            inner = jnp.where(left, sides[0], sides[1])
            z = g_ref[at, lanes].astype(F32)
            skip = jnp.where(left[0:1, :], skip_ref[2 * p], skip_ref[2 * p + 1])
            gated = (inner + carried + skip * xp.astype(F32)) * (
                z * (0.5 * jnp.tanh(0.5 * z) + 0.5)
            )
            acc = acc + gated * gated
            g_ref[at, lanes] = (gated * gain_ref[lanes][None, :]).astype(BF16)
        ss_buf[c] = contract(ones, acc, 1, 1, HIGH)

    if ranks == 4:
        order = [ranks - 1 - me, lax.rem(me + 2, ranks), me + 1 - 2 * lax.rem(me, 2)]
    else:
        order = [lax.rem(me + k, ranks) for k in range(1, ranks)]
    def one(t, carry):
        j = lax.div(t, ranks - 1)
        index = lax.rem(t, ranks - 1)
        dest = jnp.int32(0)
        for i, value in enumerate(order):
            dest = dest + jnp.where(index == i, value, 0)
        span(dest * each + j)
        for copy in copies(dest, j, lax.rem(me - dest + ranks, ranks) - 1):
            copy.start()
        return carry

    lax.fori_loop(0, 2, one, 0)
    move(3)
    spread_out(True)
    lax.fori_loop(2, each * (ranks - 1), one, 0)

    def mine(j, carry):
        span(me * each + j)
        return carry

    lax.fori_loop(0, each, mine, 0)

    def wait_ws(i, carry):
        load_w(i).wait()
        return carry

    lax.fori_loop(1, shards, wait_ws, 0)
    local = pl.ds(pl.multiple_of(me * share, share), share)

    def own_tile(n, carry):
        lanes = pl.ds(pl.multiple_of(n * TILE, TILE), TILE)
        acc_ref[:, lanes] = jnp.dot(
            g_ref[local, :], w_ref[me, :, lanes], preferred_element_type=F32
        )
        return carry

    lax.fori_loop(0, tiles, own_tile, 0)

    near = near_order(ranks)
    late = late_order(ranks)

    def source_of(table, i):
        return pick([row[i] for row in table], me)

    def pass_direct(i):
        r = source_of(near, i)
        if square:
            for j in direct:
                landed(r, j).wait_recv()
                turn(r, j - 1).start()
                across(r, j, core).start()
        else:

            def one(j):
                landed(r, j).wait_recv()
                across(r, j, core).start()

            over_chips(1, one)

    def pass_corner(i):
        r = source_of(near, i)
        if square:
            for part in (0, 1):
                turned(r, part).wait_recv()
            across(r, 3, core).start()
        over_chips(0, lambda j: across(r, j, 1 - core).wait_recv())

    pass_direct(0)
    spread_out(False)
    for i in range(1, ranks - 1):
        pass_direct(i)
        pass_corner(i - 1)
    pass_corner(ranks - 2)

    def take(i):
        r = source_of(late, i)
        return r, lax.rem(r - me + ranks, ranks) - 1

    def receive(r, slot, j):
        for copy in copies(r, j, slot):
            copy.wait_recv()

    for i in range(ranks - 2):
        r, slot = take(i)
        for j in range(each):
            receive(r, slot, j)

        def more(n, carry, r=r, slot=slot):
            lanes = pl.ds(pl.multiple_of(n * TILE, TILE), TILE)
            acc_ref[:, lanes] += jnp.dot(
                got_ref[slot], w_ref[r, :, lanes], preferred_element_type=F32
            )
            return carry

        lax.fori_loop(0, tiles, more, 0)

    r, slot = take(ranks - 2)
    unit = jnp.where(lax.broadcasted_iota(jnp.int32, (8, 128), 0) == 0, 1.0, 0.0).astype(F32)

    def put(n, j):
        lanes = pl.ds(pl.multiple_of(n * TILE, TILE), TILE)
        at = pl.ds(j * SPAN, SPAN)
        return pltpu.make_async_copy(
            res_ref.at[at, lanes], out_hbm.at[at, lanes], out_sem.at[n, j]
        )

    for j in range(each):
        receive(r, slot, j)
        total = ss_buf[me * each + j]
        for k in range(ranks - 1):
            total = total + ss_ref[k, j]
        column = contract(total, unit, 0, 0, HIGH) * (1.0 / (width * ranks))
        token = me * share + j * SPAN + lax.broadcasted_iota(jnp.int32, (SPAN, 128), 0)
        scale = jnp.where(token < valid, lax.rsqrt(column + 1e-05), 0.0)
        wide = jnp.concatenate([scale] * (TILE // 128), axis=1)
        at = pl.ds(j * SPAN, SPAN)

        def final(n, carry, j=j, at=at, wide=wide):
            lanes = pl.ds(pl.multiple_of(n * TILE, TILE), TILE)
            part = jnp.dot(got_ref[slot, at, :], w_ref[r, :, lanes], preferred_element_type=F32)
            res_ref[at, lanes] = ((acc_ref[at, lanes] + part) * wide).astype(BF16)
            put(n, j).start()
            return carry

        lax.fori_loop(0, tiles, final, 0)

    for h in range(ranks):

        @pl.when(me == h)
        def _(h=h):
            for r, a, b, part, phase in moves:
                if a == h:
                    along(r, b, part).wait_send()

    for i in range(ranks - 1):
        r = source_of(near, i)
        if square:
            for j in direct:
                plane(r, j).wait_send()
                turn(r, j - 1).wait_send()
        else:
            over_chips(1, lambda j: plane(r, j).wait_send())
        over_chips(0, lambda j: across(r, j, core).wait_send())

    def told(j, carry):
        @pl.when(chip + j < chips)
        def _():
            to_chip(j, chip + j).wait_send()

        return carry

    lax.fori_loop(1, chips, told, 0)
    for dest in order:
        slot = lax.rem(me - dest + ranks, ranks) - 1

        def sent(j, carry, dest=dest, slot=slot):
            for copy in copies(dest, j, slot):
                copy.wait_send()
            return carry

        lax.fori_loop(0, each, sent, 0)

    def wait_put(n, carry):
        for j in range(each):
            put(n, j).wait()
        return carry

    lax.fori_loop(0, tiles, wait_put, 0)


def body(
    ranks,
    shards,
    values,
    gates,
    b_proj,
    c_proj,
    step_size,
    decay_rate,
    skip_gain,
    norm_gain,
    readout,
    span_counts,
    remaining_count,
):
    length, width = values.shape
    heads = step_size.shape[0]
    state = b_proj.shape[1]
    depth = readout.shape[1]
    blocks = length // SPAN
    share = length // ranks
    each = blocks // ranks
    chips = shards // 2
    sds = jax.ShapeDtypeStruct
    smem = pl.BlockSpec(memory_space=pltpu.SMEM)
    hbm = pl.BlockSpec(memory_space=pl.ANY)
    dma = pltpu.SemaphoreType.DMA
    return pl.pallas_call(
        functools.partial(layer_kernel, ranks, shards),
        out_shape=sds((share, depth), BF16),
        in_specs=[smem, smem, smem, pl.BlockSpec(memory_space=VMEM)] + [hbm] * 7,
        out_specs=hbm,
        scratch_shapes=[
            VMEM((length, width), BF16),
            VMEM((length, width), BF16),
            VMEM((length, state), BF16),
            VMEM((length, state), BF16),
            VMEM((heads, length), F32),
            VMEM((heads, length), F32),
            VMEM((length, heads), F32),
            VMEM((heads, length), F32),
            VMEM((blocks, state, width), F32),
            VMEM((blocks, 8, width), F32),
            VMEM((state, width), F32),
            VMEM((8, width), F32),
            VMEM((state + 16, width), BF16),
            VMEM((state + 16, width), BF16),
            VMEM((state + 16, width // 2), BF16),
            VMEM((chips, state + 16, width // 2), BF16),
            VMEM((state, width), F32),
            VMEM((ranks, width, depth), BF16),
            VMEM((ranks - 1, share, width), BF16),
            VMEM((blocks, 8, SPAN), F32),
            VMEM((ranks - 1, each, 8, SPAN), F32),
            VMEM((share, depth), F32),
            VMEM((share, depth), BF16),
            dma((blocks,)),
            dma((blocks,)),
            dma((4,)),
            dma((shards,)),
            dma((ranks, ranks, 2)),
            dma((ranks, 2)),
            dma((ranks - 1, chips)),
            dma((ranks - 1, chips)),
            dma((ranks - 1, chips)),
            dma((ranks - 1, chips)),
            dma((2,)),
            dma((2,)),
            dma((chips,)),
            dma((chips,)),
            dma((ranks - 1, each)),
            dma((ranks - 1, each)),
            dma((ranks - 1, each)),
            dma((ranks - 1, each)),
            dma((depth // TILE, each)),
        ],
        compiler_params=pltpu.CompilerParams(
            vmem_limit_bytes=LIMIT, collective_id=0, has_side_effects=True
        ),
        cost_estimate=pl.CostEstimate(
            flops=10**11, bytes_accessed=20 * 10**6, transcendentals=0
        ),
        name="layer",
    )(
        span_counts,
        remaining_count,
        skip_gain,
        norm_gain,
        values,
        gates,
        b_proj,
        c_proj,
        step_size,
        decay_rate,
        readout,
    )


def solution(mesh):
    return jax.shard_map(
        functools.partial(body, mesh.shape["head"], mesh.shape["seq"]),
        mesh=mesh,
        in_specs=(
            P("seq", "head"),
            P("seq", "head"),
            P("seq", None),
            P("seq", None),
            P("head", "seq"),
            P("head", "seq"),
            P("head"),
            P("head"),
            P("head", None),
            P("seq"),
            P("seq"),
        ),
        out_specs=P(("seq", "head"), None),
        check_vma=False,
    )
```
